32 devices in a mesh: scan: 4 (over y, core), ascan: 8 (over z, x).
Axes of the slice: x: 2, y: 2, z: 4, core: 2. Of those that a mesh axis runs over, the one named last changes fastest.
Arguments:
- spectra: bfloat16 [8, 4, 1024, 2048], P('scan', None, 'ascan'), may hold values from -8 to 8
- surface_top: int32 [8, 1024], P('scan', 'ascan'), may hold values from 0 to 3, as said below
- surface_bottom: int32 [8, 1024], P('scan', 'ascan'), may hold values from 1 to 8, as said below
Outputs:
- angiogram: float32 [8, 1024, 1024], P('scan', 'ascan')
- structure_map: float32 [8, 1024, 1024], P('scan', 'ascan')
- speckle_map: float32 [8, 1024, 1024], P('scan', 'ascan')
- mean_flow: float32 [], replicated
The draws below stay inside these ranges and needn't reach their ends.
Inputs may be any that keep to these rules, and one draw needn't show every extreme that they name: surface_top counts tiles of 128 depth rows. surface_bottom is greater than surface_top of the same A-scan.
All inputs are finite; a program needn't handle non-finite values.
Results may differ from the reference program's by a relative error of at most 0.0032.
Values sent between devices are 32-bit elements; how exact they have to be, the bound alone decides.
No kernel may reach another device: no remote copies, remote signals or barrier semaphores. Data moves between devices by JAX's collectives and lax.ppermute only.
A program may use at most 128 MiB of HBM per device.

```python
import math
import jax
import jax.numpy as jnp
from jax import lax

REPEATS = 4
BINS = 2048
BANDS = 4
TILE = 128
BAND_BINS = 512
DEPTH = 1024
TILES = 8
NBSCAN = 8
ASCANS = 1024


def surfaces(key):
    first_key = jax.random.fold_in(key, 101)
    second_key = jax.random.fold_in(key, 202)
    surface_top = jax.random.randint(first_key, (NBSCAN, ASCANS), 0, TILES // 2, dtype=jnp.int32)
    position = jnp.arange(ASCANS, dtype=jnp.int32)[None, :]
    room_left = TILES - surface_top
    reach = 1 + (room_left - 1) * (position + 1) // ASCANS
    thickness = jax.random.randint(second_key, (NBSCAN, ASCANS), 1, reach + 1, dtype=jnp.int32)
    return (surface_top, surface_top + thickness)


def draw_surface_top(key, part):
    return surfaces(key)[0]


def draw_surface_bottom(key, part):
    return surfaces(key)[1]


def draw_spectra(key, part):
    phase_key = jax.random.fold_in(key, 303)
    stripe_key = jax.random.fold_in(key, 404)
    common_key = jax.random.fold_in(key, 505)
    own_key = jax.random.fold_in(key, 606)
    phase_shift = jax.random.uniform(phase_key, (NBSCAN, 1), jnp.float32)
    position = jnp.arange(ASCANS, dtype=jnp.float32)[None, :] / ASCANS
    wave = jnp.sin(2.0 * math.pi * (position + phase_shift))
    correlation = 0.5 + 0.45 * wave
    vessel = jax.random.bernoulli(stripe_key, 0.15, (NBSCAN, ASCANS))
    correlation = jnp.where(vessel, 0.0, correlation)
    shared_part = jnp.sqrt(correlation)[:, None, :, None]
    own_part = jnp.sqrt(1.0 - correlation)[:, None, :, None]
    common = jax.random.normal(common_key, (NBSCAN, 1, ASCANS, BINS), jnp.float32)
    own = jax.random.normal(own_key, (NBSCAN, REPEATS, ASCANS, BINS), jnp.float32)
    mixed = jnp.clip(shared_part * common + own_part * own, -6.0, 6.0)
    return mixed.astype(jnp.bfloat16)


def setup_inputs(seed: int = 0) -> dict:
    keys = jax.random.split(jax.random.key(seed), 4)
    return {
        "spectra": draw_spectra(jax.random.fold_in(keys[3], 71), 0),
        "surface_top": draw_surface_top(jax.random.fold_in(keys[3], 71), 0),
        "surface_bottom": draw_surface_bottom(jax.random.fold_in(keys[3], 71), 0),
    }


FLOOR_SHARE = 0.05
VARIANCE_SCALE = 0.1

def make_table():
    sample = jnp.arange(BAND_BINS, dtype=jnp.int32)
    depth_index = jnp.arange(DEPTH, dtype=jnp.int32)
    product = sample[:, None] * depth_index[None, :] % BINS
    phase_angle = product.astype(jnp.float32) * (2.0 * math.pi / BINS)
    window = jnp.sin(math.pi * (sample.astype(jnp.float32) + 0.5) / BAND_BINS) ** 2
    cosine = window[:, None] * jnp.cos(phase_angle)
    sine = window[:, None] * jnp.sin(phase_angle)
    return jnp.concatenate([cosine, sine], axis=1).astype(jnp.bfloat16)

def band_moments(spectra, table_part, first_row, surface_top, surface_bottom):
    scan_count, repeat_count, ascan_count, bin_count = spectra.shape
    depth_width = table_part.shape[1] // 2
    flat = spectra.reshape(scan_count * repeat_count * ascan_count, BANDS, BAND_BINS)
    similarity_total = jnp.zeros((scan_count, ascan_count, depth_width), jnp.float32)
    amplitude_total = jnp.zeros((scan_count, ascan_count, depth_width), jnp.float32)
    variance_total = jnp.zeros((scan_count, ascan_count, depth_width), jnp.float32)
    for band_index in range(BANDS):
        profile = jnp.dot(flat[:, band_index, :], table_part, preferred_element_type=jnp.float32)
        profile = profile.reshape(scan_count, repeat_count, ascan_count, 2 * depth_width)
        amplitude = jnp.sqrt(profile[..., :depth_width] ** 2 + profile[..., depth_width:] ** 2)
        earlier = amplitude[:, :-1]
        later = amplitude[:, 1:]
        similarity = 2.0 * earlier * later / jnp.maximum(earlier ** 2 + later ** 2, FLOOR_SHARE * BAND_BINS)
        similarity_total = similarity_total + lax.optimization_barrier(jnp.sum(similarity, axis=1))
        amplitude_total = amplitude_total + lax.optimization_barrier(jnp.sum(amplitude, axis=1))
        repeat_mean = lax.optimization_barrier(jnp.mean(amplitude, axis=1, keepdims=True))
        variance_total = variance_total + lax.optimization_barrier(jnp.mean((amplitude - repeat_mean) ** 2, axis=1))
    depth_rows = first_row + jnp.arange(depth_width, dtype=jnp.int32)
    lower = depth_rows[None, None, :] >= surface_top[..., None] * TILE
    upper = depth_rows[None, None, :] < surface_bottom[..., None] * TILE
    inside = (lower & upper).astype(jnp.float32)
    decorrelation = (1.0 - similarity_total / (BANDS * (REPEATS - 1))) * inside
    structure = amplitude_total / (BANDS * REPEATS) / math.sqrt(BAND_BINS) * inside
    speckle = variance_total / BANDS / (VARIANCE_SCALE * BAND_BINS) * inside
    return (decorrelation, structure, speckle, jnp.sum(decorrelation), jnp.sum(inside))

def reference(spectra, surface_top, surface_bottom):
    dft_table = make_table()

    def one_scan(items):
        scan_spectra, scan_top, scan_bottom = items
        return band_moments(scan_spectra[None], dft_table, 0, scan_top[None], scan_bottom[None])
    decorrelation, structure, speckle, flow_sums, tissue_counts = lax.map(one_scan, (spectra, surface_top, surface_bottom))
    decorrelation = decorrelation[:, 0]
    structure = structure[:, 0]
    speckle = speckle[:, 0]
    mean_flow = jnp.sum(flow_sums) / jnp.sum(tissue_counts)
    padded = jnp.pad(decorrelation, ((0, 0), (1, 1), (0, 0)))
    smoothed = (padded[:, :-2] + padded[:, 1:-1] + padded[:, 2:]) / 3.0
    angiogram = jnp.swapaxes(smoothed / mean_flow, 1, 2)
    return (angiogram, jnp.swapaxes(structure, 1, 2), jnp.swapaxes(speckle, 1, 2), mean_flow)
```

```python
import functools
import math

import jax
import jax.numpy as jnp
import numpy as np
from jax import lax
from jax.experimental import pallas as pl
from jax.experimental.pallas import tpu as pltpu
from jax.sharding import PartitionSpec as P

REPEATS = 4
BINS = 2048
BANDS = 4
TILE = 128
BAND_BINS = 512
DEPTH = 1024
TILES = DEPTH // TILE
FLOOR = 0.05 * BAND_BINS
VARIANCE_SCALE = 0.1
HEAD = 8
MAPS = 3


def table_values():
    sample = np.arange(BAND_BINS)
    depth = np.arange(DEPTH)
    product = (sample[:, None] * depth[None, :]) % BINS
    angle = product.astype(np.float32) * np.float32(2.0 * math.pi / BINS)
    window = np.sin(np.float32(math.pi) * (sample.astype(np.float32) + 0.5) / BAND_BINS) ** 2
    return window[:, None] * np.cos(angle), window[:, None] * np.sin(angle)


def tile_tables(width):
    cosine, sine = table_values()
    slabs = DEPTH // width
    cosine = cosine.reshape(BAND_BINS, slabs, width)
    sine = sine.reshape(BAND_BINS, slabs, width)
    both = np.concatenate([cosine, sine], axis=2).transpose(1, 0, 2)
    return jnp.asarray(both.astype(np.float32)).astype(jnp.bfloat16)


def moments_rows(profile_ref, buf, out_ref, slot, scan, ascans):
    tiny = jnp.float32(np.finfo(np.float32).tiny)
    step = 8
    for start in range(0, ascans, step):
        sim = amp = var1 = var2 = None
        for band in range(BANDS):
            power, amplitude = [], []
            for repeat in range(REPEATS):
                base = repeat * ascans + start
                re = profile_ref[buf, band, base : base + step, :TILE]
                im = profile_ref[buf, band, base : base + step, TILE:]
                p = re * re + im * im
                power.append(p)
                amplitude.append(p * lax.rsqrt(jnp.maximum(p, tiny)))
            parts = []
            for r in range(REPEATS - 1):
                root = lax.rsqrt(jnp.maximum(power[r] + power[r + 1], FLOOR))
                parts.append((amplitude[r] * root) * (amplitude[r + 1] * root))
            s = parts[0] + parts[1] + parts[2]
            s01 = amplitude[0] + amplitude[1]
            s23 = amplitude[2] + amplitude[3]
            d01 = amplitude[0] - amplitude[1]
            d23 = amplitude[2] - amplitude[3]
            a = s01 + s23
            d = s01 - s23
            v1 = d01 * d01 + d23 * d23
            v2 = d * d
            sim = s if sim is None else sim + s
            amp = a if amp is None else amp + a
            var1 = v1 if var1 is None else var1 + v1
            var2 = v2 if var2 is None else var2 + v2
        rows = pl.ds(scan * ascans + start, step)
        out_ref[slot, rows, 0:TILE] = 1.0 - sim * (2.0 / (BANDS * (REPEATS - 1)))
        out_ref[slot, rows, TILE : 2 * TILE] = amp * (1.0 / (BANDS * REPEATS * math.sqrt(BAND_BINS)))
        out_ref[slot, rows, 2 * TILE :] = (var1 + 0.5 * var2) * (
            0.5 / (REPEATS * BANDS * VARIANCE_SCALE * BAND_BINS)
        )


def split(x):
    high = x.astype(jnp.bfloat16)
    low = (x - high.astype(jnp.float32)).astype(jnp.bfloat16)
    return high, low


def tissue(top, bottom, tile):
    rows = top.shape[1]
    mask = jnp.where((top <= tile) & (tile < bottom), 1.0, 0.0).astype(jnp.float32)
    before = lax.broadcasted_iota(jnp.int32, (rows, rows), 0) < lax.broadcasted_iota(
        jnp.int32, (rows, rows), 1
    )
    spread = jnp.broadcast_to(mask, (8, rows)).astype(jnp.bfloat16)
    rank = jnp.dot(spread, before.astype(jnp.bfloat16), preferred_element_type=jnp.float32)[0:1]
    return mask, jnp.where(mask > 0.0, rank, -1.0).astype(jnp.int32)


def chooser(rank, first, count):
    rows = rank.shape[1]
    index = lax.broadcasted_iota(jnp.int32, (count, rows), 0) + first
    return jnp.where(index == rank, 1.0, 0.0).astype(jnp.bfloat16)


def flat_rows(block):
    return jnp.concatenate([block[i : i + 1] for i in range(block.shape[0])], axis=1)


def send_kernel(levels, order_ref, x_ref, table_ref, top_ref, bottom_ref, *refs):
    outs = refs[: sum(len(l) for l in levels)]
    flow_ref, profile_ref, maps_ref = refs[len(outs) :]
    slots = len(levels)
    scans, _, ascans, _ = x_ref.shape
    last = slots * scans

    def product(slot, scan, buf):
        weights = table_ref[order_ref[slot]]
        for band in range(BANDS):
            lanes = slice(band * BAND_BINS, (band + 1) * BAND_BINS)
            x = x_ref[scan, :, :, lanes].reshape(REPEATS * ascans, BAND_BINS)
            profile_ref[buf, band] = jnp.dot(x, weights, preferred_element_type=jnp.float32)

    product(0, 0, 0)

    def step(slot, carry):
        for scan in range(scans):
            following = jnp.minimum(slot + 1, slots - 1) if scan == scans - 1 else slot
            product(following, (scan + 1) % scans, (scan + 1) % 2)
            moments_rows(profile_ref, scan % 2, maps_ref, slot, scan, ascans)
        return carry

    lax.fori_loop(0, slots, step, 0)

    top = flat_rows(top_ref[...])
    bottom = flat_rows(bottom_ref[...])
    rows = top.shape[1]
    flow = jnp.zeros((1, TILE), jnp.float32)
    position = 0
    for slot, sizes in enumerate(levels):
        mask, rank = tissue(top, bottom, order_ref[slot])
        maps = maps_ref[slot]
        high, low = split(maps)
        spread = jnp.broadcast_to(mask, (8, rows)).astype(jnp.bfloat16)
        flow += (
            jnp.dot(spread, high[:, :TILE], preferred_element_type=jnp.float32)
            + jnp.dot(spread, low[:, :TILE], preferred_element_type=jnp.float32)
        )[0:1]
        first = 0
        for level, (count, head) in enumerate(sizes):
            out = outs[position]
            position += 1
            if head:
                out[0:HEAD, :] = jnp.zeros((HEAD, MAPS * TILE), jnp.float32)
                out[0:1, 0:rows] = top.astype(jnp.float32)
                out[1:2, 0:rows] = bottom.astype(jnp.float32)
            pick = chooser(rank, first, count)
            out[head : head + count, :] = jnp.dot(
                pick, high, preferred_element_type=jnp.float32
            ) + jnp.dot(pick, low, preferred_element_type=jnp.float32)
            first += count
    flow_ref[...] = jnp.broadcast_to(flow, flow_ref.shape)


VMEM = pl.BlockSpec(memory_space=pltpu.VMEM)
SMEM = pl.BlockSpec(memory_space=pltpu.SMEM)


def send(order, spectra, tables, top, bottom, levels, name):
    scans, repeats, ascans, bins = spectra.shape
    assert scans % 2 == 0
    rows = scans * ascans
    shapes = [
        jax.ShapeDtypeStruct((head + count, MAPS * TILE), jnp.float32)
        for sizes in levels
        for count, head in sizes
    ]
    shapes.append(jax.ShapeDtypeStruct((8, TILE), jnp.float32))
    flops = 2 * rows * repeats * bins * 2 * TILE * len(levels)
    return pl.pallas_call(
        functools.partial(send_kernel, levels),
        out_shape=shapes,
        in_specs=[SMEM, VMEM, VMEM, VMEM, VMEM],
        out_specs=[VMEM] * len(shapes),
        scratch_shapes=[
            pltpu.VMEM((2, BANDS, repeats * ascans, 2 * TILE), jnp.float32),
            pltpu.VMEM((len(levels), rows, MAPS * TILE), jnp.float32),
        ],
        cost_estimate=pl.CostEstimate(
            flops=flops, bytes_accessed=2 * spectra.size, transcendentals=0
        ),
        compiler_params=pltpu.CompilerParams(vmem_limit_bytes=48 * 1024 * 1024),
        name=name,
    )(order, spectra, tables, top, bottom)


def receive_kernel(levels, source_ref, mean_ref, top_ref, bottom_ref, *refs):
    count = sum(len(l) for l in levels)
    ins = refs[:count]
    angiogram_ref, structure_ref, speckle_ref, decorrelation_ref = refs[count:]
    scans = angiogram_ref.shape[0]
    total = angiogram_ref.shape[2]
    own_top = flat_rows(top_ref[...])
    own_bottom = flat_rows(bottom_ref[...])
    ascans = own_top.shape[1] // scans
    tile = source_ref[len(levels)]
    position = 0
    for slot, sizes in enumerate(levels):
        pieces = ins[position : position + len(sizes)]
        position += len(sizes)
        if sizes[0][1]:
            top = pieces[0][0:1, 0 : scans * ascans].astype(jnp.int32)
            bottom = pieces[0][1:2, 0 : scans * ascans].astype(jnp.int32)
        else:
            top, bottom = own_top, own_bottom
        _, rank = tissue(top, bottom, tile)
        first = 0
        result = None
        for piece, (rows, head) in zip(pieces, sizes):
            pick = chooser(rank, first, rows)
            first += rows
            for part in split(piece[head : head + rows, :]):
                term = lax.dot_general(
                    part, pick, (((0,), (0,)), ((), ())), preferred_element_type=jnp.float32
                )
                result = term if result is None else result + term
        lanes = pl.ds(pl.multiple_of(source_ref[slot] * ascans, ascans), ascans)
        for scan in range(scans):
            columns = slice(scan * ascans, (scan + 1) * ascans)
            decorrelation_ref[scan, :, lanes] = result[0:TILE, columns]
            structure_ref[scan, :, lanes] = result[TILE : 2 * TILE, columns]
            speckle_ref[scan, :, lanes] = result[2 * TILE :, columns]
    scale = 1.0 / (3.0 * mean_ref[0:1, 0:1])
    step = 8
    for scan in range(scans):
        for start in range(0, TILE, step):
            d = decorrelation_ref[scan, start : start + step, :]
            lane = lax.broadcasted_iota(jnp.int32, d.shape, 1)
            left = jnp.where(lane == 0, 0.0, pltpu.roll(d, 1, 1))
            right = jnp.where(lane == total - 1, 0.0, pltpu.roll(d, total - 1, 1))
            angiogram_ref[scan, start : start + step, :] = ((left + d) + right) * scale


def receive(source, mean, top, bottom, pieces, levels, members, name):
    scans, ascans = top.shape
    shape = jax.ShapeDtypeStruct((scans, TILE, members * ascans), jnp.float32)
    return pl.pallas_call(
        functools.partial(receive_kernel, levels),
        out_shape=[shape] * MAPS,
        in_specs=[SMEM] + [VMEM] * (3 + len(pieces)),
        out_specs=[VMEM] * MAPS,
        scratch_shapes=[pltpu.VMEM(shape.shape, jnp.float32)],
        cost_estimate=pl.CostEstimate(
            flops=2 * 2 * scans * ascans * 256 * MAPS * TILE * members,
            bytes_accessed=8 * MAPS * scans * TILE * members * ascans,
            transcendentals=0,
        ),
        compiler_params=pltpu.CompilerParams(vmem_limit_bytes=48 * 1024 * 1024),
        name=name,
    )(source, mean, top, bottom, *pieces)


def capacities(members, scans, ascans):
    total = members * ascans
    position = np.arange(total)
    chance = np.zeros((total, TILES))
    half = TILES // 2
    for top in range(half):
        reach = 1 + (TILES - top - 1) * (position + 1) // total
        for tile in range(top, TILES):
            chance[:, tile] += np.clip(reach - (tile - top), 0, None) / reach / half
    mean = chance.reshape(members, ascans, TILES).sum(1) * scans
    spread = np.sqrt((chance * (1 - chance)).reshape(members, ascans, TILES).sum(1) * scans)
    caps = np.ceil((mean + 4.0 * spread + 0.5) / 8) * 8
    return np.minimum(caps, scans * ascans).astype(int)


def matchings(members):
    half = members // 2
    far = [
        [(s + half) % members // half * half + (s % half + m) % half for s in range(members)]
        for m in range(half)
    ]
    near = [[s // half * half + ((s % half) ^ j) for s in range(members)] for j in range(1, half)]
    return far, near


def plan_levels(caps, matching, merge):
    need = [int(caps[s, d]) for s, d in enumerate(matching)]
    base = sorted(need)[len(need) // 2]
    need = [max(n, base) for n in need]
    marks = []
    for value in sorted(set(need)):
        if len(marks) > 1 and value - marks[-1] < merge:
            marks[-1] = value
        else:
            marks.append(value)
    plan, covered, below = [], [0] * len(need), 0
    for mark in marks:
        pairs = [(s, d) for s, d in enumerate(matching) if need[s] > below]
        for s, _ in pairs:
            covered[s] = mark
        plan.append((mark - below, pairs))
        below = mark
    return plan, covered


def sparse_body(members, spectra, top, bottom):
    scans, repeats, ascans, bins = spectra.shape
    rows = scans * ascans
    me = lax.axis_index("ascan")
    tables = tile_tables(TILE)
    far, near = matchings(members)
    caps = capacities(members, scans, ascans)
    far_plans = [plan_far(caps, m) for m in far]
    near_cap = max(int(caps[s, d]) for m in near for s, d in enumerate(m))
    near_plans = [([(near_cap, list(enumerate(m)))], [near_cap] * members) for m in near]

    def target(matching):
        return jnp.asarray(np.array(matching, np.int32))[me]

    def origin(matching):
        inverse = np.argsort(np.array(matching)).astype(np.int32)
        return jnp.asarray(inverse)[me]

    room = np.zeros((members, TILES), np.int32)
    for matching, (plan, covered) in list(zip(far, far_plans)) + list(zip(near, near_plans)):
        for s, d in enumerate(matching):
            room[s, d] = covered[s]
    for s in range(members):
        room[s, s] = rows
    tiles = jnp.arange(TILES, dtype=jnp.int32)[:, None]
    flat_top, flat_bottom = top.reshape(1, rows), bottom.reshape(1, rows)
    need = jnp.sum(((flat_top <= tiles) & (tiles < flat_bottom)).astype(jnp.int32), axis=1)
    over = jnp.any(need > jnp.asarray(room)[me]).astype(jnp.float32)

    far_levels = [
        tuple((count, HEAD if i == 0 else 0) for i, (count, _) in enumerate(plan))
        for plan, _ in far_plans
    ]
    near_levels = [((near_cap, HEAD),) for _ in near]
    own_level = ((rows, 0),)

    far_order = jnp.stack([target(m) for m in far]).astype(jnp.int32)
    near_order = jnp.stack([target(m) for m in near] + [me]).astype(jnp.int32)
    *far_out, far_flow = send(far_order, spectra, tables, top, bottom, far_levels, "far_tiles")
    received, position = [], 0
    by_level = []
    for plan, _ in far_plans:
        for level, (_, pairs) in enumerate(plan):
            by_level.append((level, position, pairs))
            position += 1
    received = [None] * position
    for level, index, pairs in sorted(by_level, key=lambda item: item[0]):
        received[index] = lax.ppermute(far_out[index], "ascan", pairs)
    *near_out, near_flow = send(
        near_order, spectra, tables, top, bottom, near_levels + [own_level], "near_tiles"
    )
    for (plan, _), message in zip(near_plans, near_out):
        received.append(lax.ppermute(message, "ascan", plan[0][1]))
    received.append(near_out[-1])

    flow = jnp.sum(far_flow[0] + near_flow[0])
    count = jnp.sum(
        (jnp.minimum(bottom, TILES) - jnp.clip(top, 0, TILES)).astype(jnp.float32)
    ) * TILE
    totals = jnp.stack([flow, count, over])
    totals = jnp.pad(totals[None, :], ((0, 7), (0, 125)))
    for axis, size in (("scan", lax.axis_size("scan")), ("ascan", members)):
        stride = 1
        while stride < size:
            totals = totals + lax.ppermute(totals, axis, [(s, s ^ stride) for s in range(size)])
            stride *= 2
    mean_flow = totals[0, 0] / totals[0, 1]
    mean = jnp.full((8, TILE), 1.0, jnp.float32) * mean_flow

    source = jnp.stack([origin(m) for m in far] + [origin(m) for m in near] + [me, me]).astype(jnp.int32)

    def quick(received):
        return tuple(
            receive(
                source,
                mean,
                top,
                bottom,
                received,
                far_levels + near_levels + [own_level],
                members,
                "receive_tiles",
            )
        )

    def dense(received):
        everyone = jnp.arange(TILES, dtype=jnp.int32)
        halves = []
        for part in (everyone[: TILES // 2], everyone[TILES // 2 :]):
            *out, _ = send(
                part, spectra, tables, top, bottom, [((rows, HEAD),)] * (TILES // 2), "dense_tiles"
            )
            halves += out
        swapped = lax.all_to_all(jnp.stack(halves), "ascan", 0, 0, tiled=True)
        return tuple(
            receive(
                jnp.concatenate([everyone, me[None].astype(jnp.int32)]),
                mean,
                top,
                bottom,
                [swapped[i] for i in range(members)],
                [((rows, HEAD),)] * members,
                members,
                "dense_receive",
            )
        )

    outs = lax.cond(totals[0, 2] > 0.0, dense, quick, received)
    return (*outs, mean_flow)


def plan_far(caps, matching):
    return plan_levels(caps, matching, 40)


def plain_body(spectra, surface_top, surface_bottom):
    scans, repeats, ascans, bins = spectra.shape
    cosine, sine = table_values()
    table = jnp.asarray(np.concatenate([cosine, sine], axis=1).astype(np.float32)).astype(jnp.bfloat16)
    similarity = amplitude_sum = variance = jnp.zeros((scans, ascans, DEPTH), jnp.float32)
    for band in range(BANDS):
        part = spectra[..., band * BAND_BINS : (band + 1) * BAND_BINS]
        profile = jnp.dot(part.reshape(-1, BAND_BINS), table, preferred_element_type=jnp.float32)
        profile = profile.reshape(scans, repeats, ascans, 2 * DEPTH)
        amplitude = jnp.sqrt(profile[..., :DEPTH] ** 2 + profile[..., DEPTH:] ** 2)
        first, second = amplitude[:, :-1], amplitude[:, 1:]
        similarity += jnp.sum(
            2.0 * first * second / jnp.maximum(first**2 + second**2, FLOOR), axis=1
        )
        amplitude_sum += jnp.sum(amplitude, axis=1)
        center = jnp.mean(amplitude, axis=1, keepdims=True)
        variance += jnp.mean((amplitude - center) ** 2, axis=1)
    depth = jnp.arange(DEPTH, dtype=jnp.int32)
    inside = (depth >= surface_top[..., None] * TILE) & (depth < surface_bottom[..., None] * TILE)
    inside = inside.astype(jnp.float32)
    decorrelation = (1.0 - similarity / (BANDS * (REPEATS - 1))) * inside
    structure = amplitude_sum / (BANDS * REPEATS) / math.sqrt(BAND_BINS) * inside
    speckle = variance / BANDS / (VARIANCE_SCALE * BAND_BINS) * inside
    totals = lax.psum((jnp.sum(decorrelation), jnp.sum(inside)), ("scan", "ascan"))
    mean_flow = totals[0] / totals[1]
    decorrelation, structure, speckle = (
        lax.all_to_all(x, "ascan", split_axis=2, concat_axis=1, tiled=True)
        for x in (decorrelation, structure, speckle)
    )
    padded = jnp.pad(decorrelation, ((0, 0), (1, 1), (0, 0)))
    smoothed = (padded[:, :-2] + padded[:, 1:-1] + padded[:, 2:]) / 3.0
    angiogram = jnp.swapaxes(smoothed / mean_flow, 1, 2)
    return (angiogram, jnp.swapaxes(structure, 1, 2), jnp.swapaxes(speckle, 1, 2), mean_flow)


def solution(mesh):
    members = mesh.shape["ascan"]
    scans = mesh.shape["scan"]

    def body(spectra, surface_top, surface_bottom):
        local_scans, _, ascans, _ = spectra.shape
        fits = (
            members == TILES
            and scans & (scans - 1) == 0
            and local_scans % 2 == 0
            and ascans == TILE
            and local_scans * ascans <= MAPS * TILE
        )
        if fits:
            return sparse_body(members, spectra, surface_top, surface_bottom)
        return plain_body(spectra, surface_top, surface_bottom)

    return jax.shard_map(
        body,
        mesh=mesh,
        in_specs=(P("scan", None, "ascan", None), P("scan", "ascan"), P("scan", "ascan")),
        out_specs=(
            P("scan", "ascan", None),
            P("scan", "ascan", None),
            P("scan", "ascan", None),
            P(),
        ),
        check_vma=False,
    )
```

```python
import functools
import math

import jax
import jax.numpy as jnp
import numpy as np
from jax import lax
from jax.experimental import pallas as pl
from jax.experimental.pallas import tpu as pltpu
from jax.sharding import PartitionSpec as P


REPEATS = 4
BINS = 2048
BANDS = 4
TILE = 128
BAND_BINS = 512
DEPTH = 1024
TILES = DEPTH // TILE
FLOOR = 0.05 * BAND_BINS
VARIANCE_SCALE = 0.1
HEAD = 2
MAPS = 3


def table_values():
    sample = np.arange(BAND_BINS)
    depth = np.arange(DEPTH)
    product = (sample[:, None] * depth[None, :]) % BINS
    angle = product.astype(np.float32) * np.float32(2.0 * math.pi / BINS)
    window = np.sin(np.float32(math.pi) * (sample.astype(np.float32) + 0.5) / BAND_BINS) ** 2
    return window[:, None] * np.cos(angle), window[:, None] * np.sin(angle)


def tile_tables(width):
    cosine, sine = table_values()
    slabs = DEPTH // width
    cosine = cosine.reshape(BAND_BINS, slabs, width)
    sine = sine.reshape(BAND_BINS, slabs, width)
    both = np.concatenate([cosine, sine], axis=2).transpose(1, 0, 2)
    return jnp.asarray(both.astype(np.float32)).astype(jnp.bfloat16)


def moments_rows(profile_ref, buf, out_ref, slot, scan, ascans, begin, end):
    tiny = jnp.float32(np.finfo(np.float32).tiny)
    step = 8
    for start in range(begin, end, step):
        sim = amp = var1 = var2 = None
        for band in range(BANDS):
            power, amplitude = [], []
            for repeat in range(REPEATS):
                base = repeat * ascans + start
                re = profile_ref[buf, band, base : base + step, :TILE]
                im = profile_ref[buf, band, base : base + step, TILE:]
                p = re * re + im * im
                power.append(p)
                amplitude.append(p * lax.rsqrt(jnp.maximum(p, tiny)))
            parts = []
            for r in range(REPEATS - 1):
                root = lax.rsqrt(jnp.maximum(power[r] + power[r + 1], FLOOR))
                parts.append((amplitude[r] * root) * (amplitude[r + 1] * root))
            s = parts[0] + parts[1] + parts[2]
            s01 = amplitude[0] + amplitude[1]
            s23 = amplitude[2] + amplitude[3]
            d01 = amplitude[0] - amplitude[1]
            d23 = amplitude[2] - amplitude[3]
            a = s01 + s23
            d = s01 - s23
            v1 = d01 * d01 + d23 * d23
            v2 = d * d
            sim = s if sim is None else sim + s
            amp = a if amp is None else amp + a
            var1 = v1 if var1 is None else var1 + v1
            var2 = v2 if var2 is None else var2 + v2
        rows = pl.ds(scan * ascans + start, step)
        out_ref[slot, rows, 0:TILE] = 1.0 - sim * (2.0 / (BANDS * (REPEATS - 1)))
        out_ref[slot, rows, TILE : 2 * TILE] = amp * (1.0 / (BANDS * REPEATS * math.sqrt(BAND_BINS)))
        out_ref[slot, rows, 2 * TILE :] = (var1 + 0.5 * var2) * (
            0.5 / (REPEATS * BANDS * VARIANCE_SCALE * BAND_BINS)
        )


def split(x):
    high = x.astype(jnp.bfloat16)
    low = (x - high.astype(jnp.float32)).astype(jnp.bfloat16)
    return high, low


def tissue(top, bottom, tile):
    rows = top.shape[1]
    mask = jnp.where((top <= tile) & (tile < bottom), 1.0, 0.0).astype(jnp.float32)
    before = lax.broadcasted_iota(jnp.int32, (rows, rows), 0) < lax.broadcasted_iota(
        jnp.int32, (rows, rows), 1
    )
    spread = jnp.broadcast_to(mask, (8, rows)).astype(jnp.bfloat16)
    rank = jnp.dot(spread, before.astype(jnp.bfloat16), preferred_element_type=jnp.float32)[0:1]
    return mask, jnp.where(mask > 0.0, rank, -1.0).astype(jnp.int32)


def chooser(rank, first, count):
    rows = rank.shape[1]
    index = lax.broadcasted_iota(jnp.int32, (count, rows), 0) + first
    return jnp.where(index == rank, 1.0, 0.0).astype(jnp.bfloat16)


def flat_rows(block):
    return jnp.concatenate([block[i : i + 1] for i in range(block.shape[0])], axis=1)


def peer_target(peer, me, half):
    kind, index = peer
    if kind == "far":
        return ((me & half) ^ half) | ((me + index) & (half - 1))
    return me ^ index if kind == "near" else index


def peer_origin(peer, me, half):
    kind, index = peer
    if kind == "far":
        return ((me & half) ^ half) | ((me + half - index) & (half - 1))
    return me ^ index if kind == "near" else index


def send_kernel(peers, messages, rooms, x_ref, table_ref, top_ref, bottom_ref, stats_in, *refs):
    outs = refs[: sum(len(m) for m in messages)]
    stats_ref, profile_ref, maps_ref = refs[len(outs) :]
    slots = len(peers)
    scans, _, ascans, _ = x_ref.shape
    me = lax.axis_index("ascan")
    half = lax.axis_size("ascan") // 2
    tiles = [jnp.asarray(peer_target(p, me, half), jnp.int32) for p in peers]

    def pick(slot):
        if isinstance(slot, int):
            return tiles[slot]
        chosen = tiles[0]
        for i in range(1, slots):
            chosen = jnp.where(slot == i, tiles[i], chosen)
        return chosen

    def product(weights, scan, buf, band):
        lanes = slice(band * BAND_BINS, (band + 1) * BAND_BINS)
        x = x_ref[scan, :, :, lanes].reshape(REPEATS * ascans, BAND_BINS)
        profile_ref[buf, band] = jnp.dot(x, weights, preferred_element_type=jnp.float32)

    def both(following, current):
        weights = table_ref[pick(following[0])] if following else None
        share = ascans // BANDS
        for band in range(BANDS):
            if following:
                product(weights, following[1], following[1] % 2, band)
            if current:
                moments_rows(
                    profile_ref, current[1] % 2, maps_ref, *current, ascans, band * share, (band + 1) * share
                )

    if slots == 1:
        both((0, 0), None)
        for scan in range(scans - 1):
            both((0, scan + 1), (0, scan))
        both(None, (0, scans - 1))
    else:
        both((0, 0), None)

        def step(slot, carry):
            for scan in range(scans - 1):
                both((slot, scan + 1), (slot, scan))
            both((jnp.minimum(slot + 1, slots - 1), 0), (slot, scans - 1))
            return carry

        lax.fori_loop(0, slots, step, 0)

    top = flat_rows(top_ref[...])
    bottom = flat_rows(bottom_ref[...])
    rows = top.shape[1]
    flow = jnp.zeros((8, TILE), jnp.float32)
    held = over = jnp.float32(0.0)
    position = 0
    for slot, parts in enumerate(messages):
        mask, rank = tissue(top, bottom, tiles[slot])
        high, low = split(maps_ref[slot])
        spread = jnp.broadcast_to(mask, (8, rows)).astype(jnp.bfloat16)
        flow += jnp.dot(spread, high[:, :TILE], preferred_element_type=jnp.float32)
        flow += jnp.dot(spread, low[:, :TILE], preferred_element_type=jnp.float32)
        count = jnp.sum(mask)
        held += count
        room = jnp.float32(rows)
        for source, value in enumerate(rooms[slot]):
            room = jnp.where(me == source, jnp.float32(value), room)
        over = jnp.where(count > room, 1.0, over)
        for first, size, carried, header in parts:
            out = outs[position]
            position += 1
            choice = chooser(rank, first, size)
            out[...] = jnp.dot(choice, high, preferred_element_type=jnp.float32) + jnp.dot(
                choice, low, preferred_element_type=jnp.float32
            )
            if header:
                out[carried : carried + 1, 0:rows] = top.astype(jnp.float32)
                out[carried + 1 : carried + 2, 0:rows] = bottom.astype(jnp.float32)
    line = lax.broadcasted_iota(jnp.int32, (8, TILE), 0)
    stats_ref[...] = stats_in[...] + jnp.where(
        line == 0, flow, jnp.where(line == 1, held, jnp.where(line == 2, over, 0.0))
    )


VMEM = pl.BlockSpec(memory_space=pltpu.VMEM)


def send(peers, spectra, tables, top, bottom, stats, messages, rooms):
    scans, repeats, ascans, bins = spectra.shape
    assert scans % 2 == 0
    rows = scans * ascans
    shapes = [
        jax.ShapeDtypeStruct((size, MAPS * TILE), jnp.float32)
        for parts in messages
        for _, size, _, _ in parts
    ]
    shapes.append(jax.ShapeDtypeStruct((8, TILE), jnp.float32))
    return pl.pallas_call(
        functools.partial(send_kernel, peers, messages, rooms),
        out_shape=shapes,
        in_specs=[VMEM] * 5,
        out_specs=[VMEM] * len(shapes),
        scratch_shapes=[
            pltpu.VMEM((2, BANDS, repeats * ascans, 2 * TILE), jnp.float32),
            pltpu.VMEM((len(peers), rows, MAPS * TILE), jnp.float32),
        ],
        cost_estimate=pl.CostEstimate(
            flops=2 * rows * repeats * bins * 2 * TILE * len(peers),
            bytes_accessed=2 * spectra.size,
            transcendentals=0,
        ),
        compiler_params=pltpu.CompilerParams(vmem_limit_bytes=32 * 1024 * 1024),
    )(spectra, tables, top, bottom, stats)


def receive_kernel(peers, messages, totals_ref, top_ref, bottom_ref, *refs):
    count = sum(len(m) for m in messages)
    ins = refs[:count]
    angiogram_ref, structure_ref, speckle_ref, decorrelation_ref = refs[count:]
    scans = angiogram_ref.shape[0]
    total = angiogram_ref.shape[2]
    own_top = flat_rows(top_ref[...])
    own_bottom = flat_rows(bottom_ref[...])
    rows = own_top.shape[1]
    ascans = rows // scans
    me = lax.axis_index("ascan")
    half = lax.axis_size("ascan") // 2
    position = 0
    for peer, parts in zip(peers, messages):
        pieces = ins[position : position + len(parts)]
        position += len(parts)
        top, bottom = own_top, own_bottom
        for piece, (_, _, carried, header) in zip(pieces, parts):
            if header:
                top = piece[carried : carried + 1, 0:rows].astype(jnp.int32)
                bottom = piece[carried + 1 : carried + 2, 0:rows].astype(jnp.int32)
        _, rank = tissue(top, bottom, me)
        result = None
        for piece, (first, size, carried, header) in zip(pieces, parts):
            choice = chooser(jnp.where(rank < first + carried, rank, -1), first, size)
            for part in split(piece[...]):
                term = lax.dot_general(
                    part, choice, (((0,), (0,)), ((), ())), preferred_element_type=jnp.float32
                )
                result = term if result is None else result + term
        origin = jnp.asarray(peer_origin(peer, me, half), jnp.int32)
        lanes = pl.ds(pl.multiple_of(origin * ascans, ascans), ascans)
        for scan in range(scans):
            columns = slice(scan * ascans, (scan + 1) * ascans)
            decorrelation_ref[scan, :, lanes] = result[0:TILE, columns]
            structure_ref[scan, :, lanes] = result[TILE : 2 * TILE, columns]
            speckle_ref[scan, :, lanes] = result[2 * TILE :, columns]
    flow = jnp.sum(totals_ref[0:1, :], axis=1, keepdims=True)
    scale = (totals_ref[1:2, 0:1] * TILE) / (3.0 * flow)
    step = 8
    for scan in range(scans):
        for start in range(0, TILE, step):
            d = decorrelation_ref[scan, start : start + step, :]
            lane = lax.broadcasted_iota(jnp.int32, d.shape, 1)
            left = jnp.where(lane == 0, 0.0, pltpu.roll(d, 1, 1))
            right = jnp.where(lane == total - 1, 0.0, pltpu.roll(d, total - 1, 1))
            angiogram_ref[scan, start : start + step, :] = ((left + d) + right) * scale


def receive(peers, totals, top, bottom, pieces, messages, members):
    scans, ascans = top.shape
    shape = jax.ShapeDtypeStruct((scans, TILE, members * ascans), jnp.float32)
    return pl.pallas_call(
        functools.partial(receive_kernel, peers, messages),
        out_shape=[shape] * MAPS,
        in_specs=[VMEM] * (3 + len(pieces)),
        out_specs=[VMEM] * MAPS,
        scratch_shapes=[pltpu.VMEM(shape.shape, jnp.float32)],
        cost_estimate=pl.CostEstimate(
            flops=2 * 2 * scans * ascans * 256 * MAPS * TILE * members,
            bytes_accessed=8 * MAPS * scans * TILE * members * ascans,
            transcendentals=0,
        ),
        compiler_params=pltpu.CompilerParams(vmem_limit_bytes=32 * 1024 * 1024),
    )(totals, top, bottom, *pieces)


def capacities(members, scans, ascans):
    total = members * ascans
    position = np.arange(total)
    chance = np.zeros((total, TILES))
    half = TILES // 2
    for top in range(half):
        reach = 1 + (TILES - top - 1) * (position + 1) // total
        for tile in range(top, TILES):
            chance[:, tile] += np.clip(reach - (tile - top), 0, None) / reach / half
    mean = chance.reshape(members, ascans, TILES).sum(1) * scans
    spread = np.sqrt((chance * (1 - chance)).reshape(members, ascans, TILES).sum(1) * scans)
    caps = np.ceil(mean + 3.8 * spread)
    return np.minimum(caps, scans * ascans).astype(int)


def plan_levels(caps, matching, merge):
    need = [int(caps[s, d]) + (HEAD if s != d else 0) for s, d in matching]
    base = sorted(need)[len(need) // 2]
    need = [max(n, base) for n in need]
    marks = []
    for value in sorted(set(-(-n // 8) * 8 for n in need)):
        if len(marks) > 1 and value - marks[-1] < merge:
            marks[-1] = value
        else:
            marks.append(value)
    messages, pair_lists, room, below = [], [], [0] * len(need), 0
    for mark in marks:
        pairs = [pair for pair, n in zip(matching, need) if n > below]
        head = HEAD if below == 0 else 0
        for s, _ in pairs:
            room[s] = mark - HEAD
        first = max(below - HEAD, 0)
        messages.append((first, mark - below, mark - below - head, head > 0))
        pair_lists.append(pairs)
        below = mark
    return tuple(messages), pair_lists, tuple(room)


def exchange_plans(members, scans, ascans):
    rows = scans * ascans
    half = members // 2
    caps = capacities(members, scans, ascans)
    far = [("far", m) for m in range(half)]
    near = [("near", j) for j in range(1, half)]
    own = ("near", 0)

    def pairs_of(peer):
        return [(s, int(peer_target(peer, s, half))) for s in range(members)]

    plans = {peer: plan_levels(caps, pairs_of(peer), 24) for peer in far}
    widest = max(int(caps[s, d]) for peer in near for s, d in pairs_of(peer))
    size = min(-(-(widest + HEAD) // 8) * 8, rows)
    for peer in near:
        plans[peer] = (
            ((0, size, size - HEAD, True),),
            [pairs_of(peer)],
            (size - HEAD,) * members,
        )
    plans[own] = (((0, rows, rows, False),), [None], (rows,) * members)
    return plans, far, near, own


def sparse_body(members, spectra, top, bottom):
    scans, _, ascans, _ = spectra.shape
    rows = scans * ascans
    half = members // 2
    tables = tile_tables(TILE)
    plans, far, near, own = exchange_plans(members, scans, ascans)
    stats = jnp.zeros((8, TILE), jnp.float32)
    sent = {}
    for number, group in enumerate((far[:1], far[1:2], far[2:], near + [own])):
        *out, stats = send(
            group,
            spectra,
            tables,
            top,
            bottom,
            stats,
            [plans[p][0] for p in group],
            [plans[p][2] for p in group],
        )
        for peer in group:
            for level in range(len(plans[peer][0])):
                sent[peer, level] = out.pop(0)
    received = []
    for peer in far + near + [own]:
        for level, pairs in enumerate(plans[peer][1]):
            message = sent[peer, level]
            if pairs is not None:
                message = lax.ppermute(message, "ascan", pairs)
            received.append(message)
    number = 0
    totals = stats
    for axis, length in (("scan", lax.axis_size("scan")), ("ascan", members)):
        stride = 1
        while stride < length:
            totals = totals + lax.ppermute(totals, axis, [(s, s ^ stride) for s in range(length)])
            stride *= 2
            number += 1
    mean_flow = jnp.sum(totals[0]) / (totals[1, 0] * TILE)

    def quick(received):
        peers = far + near + [own]
        messages = [plans[p][0] for p in peers]
        return tuple(receive(peers, totals, top, bottom, received, messages, members))

    def dense(received):
        everyone = [("all", t) for t in range(TILES)]
        message = ((0, rows + 8, rows, True),)
        out = []
        for part in (everyone[:half], everyone[half:]):
            *some, _ = send(
                part, spectra, tables, top, bottom, totals,
                [message] * half, [(rows,) * members] * half,
            )
            out += some
        swapped = lax.all_to_all(jnp.stack(out), "ascan", 0, 0, tiled=True)
        pieces = [swapped[i] for i in range(members)]
        return tuple(receive(everyone, totals, top, bottom, pieces, [message] * members, members))

    outs = lax.cond(totals[2, 0] > 0.0, dense, quick, received)
    return (*outs, mean_flow)


def plain_body(spectra, surface_top, surface_bottom):
    scans, repeats, ascans, _ = spectra.shape
    cosine, sine = table_values()
    table = jnp.asarray(np.concatenate([cosine, sine], axis=1).astype(np.float32)).astype(jnp.bfloat16)
    similarity = amplitude_sum = variance = jnp.zeros((scans, ascans, DEPTH), jnp.float32)
    for band in range(BANDS):
        part = spectra[..., band * BAND_BINS : (band + 1) * BAND_BINS]
        profile = jnp.dot(part.reshape(-1, BAND_BINS), table, preferred_element_type=jnp.float32)
        profile = profile.reshape(scans, repeats, ascans, 2 * DEPTH)
        amplitude = jnp.sqrt(profile[..., :DEPTH] ** 2 + profile[..., DEPTH:] ** 2)
        first, second = amplitude[:, :-1], amplitude[:, 1:]
        similarity += jnp.sum(
            2.0 * first * second / jnp.maximum(first**2 + second**2, FLOOR), axis=1
        )
        amplitude_sum += jnp.sum(amplitude, axis=1)
        center = jnp.mean(amplitude, axis=1, keepdims=True)
        variance += jnp.mean((amplitude - center) ** 2, axis=1)
    depth = jnp.arange(DEPTH, dtype=jnp.int32)
    inside = (depth >= surface_top[..., None] * TILE) & (depth < surface_bottom[..., None] * TILE)
    inside = inside.astype(jnp.float32)
    decorrelation = (1.0 - similarity / (BANDS * (REPEATS - 1))) * inside
    structure = amplitude_sum / (BANDS * REPEATS) / math.sqrt(BAND_BINS) * inside
    speckle = variance / BANDS / (VARIANCE_SCALE * BAND_BINS) * inside
    totals = lax.psum((jnp.sum(decorrelation), jnp.sum(inside)), ("scan", "ascan"))
    mean_flow = totals[0] / totals[1]
    decorrelation, structure, speckle = (
        lax.all_to_all(x, "ascan", split_axis=2, concat_axis=1, tiled=True)
        for x in (decorrelation, structure, speckle)
    )
    padded = jnp.pad(decorrelation, ((0, 0), (1, 1), (0, 0)))
    smoothed = (padded[:, :-2] + padded[:, 1:-1] + padded[:, 2:]) / 3.0
    angiogram = jnp.swapaxes(smoothed / mean_flow, 1, 2)
    return (angiogram, jnp.swapaxes(structure, 1, 2), jnp.swapaxes(speckle, 1, 2), mean_flow)


def solution(mesh):
    members = mesh.shape["ascan"]
    scans = mesh.shape["scan"]

    def fits(spectra):
        local_scans, ascans = spectra.shape[0] // scans, spectra.shape[2] // members
        return (
            members == TILES
            and scans & (scans - 1) == 0
            and local_scans % 2 == 0
            and ascans == TILE
            and local_scans * ascans <= MAPS * TILE
        )

    def program(spectra, surface_top, surface_bottom):
        sparse = fits(spectra)
        body = functools.partial(sparse_body, members) if sparse else plain_body
        step = jax.shard_map(
            body,
            mesh=mesh,
            in_specs=(P("scan", None, "ascan", None), P("scan", "ascan"), P("scan", "ascan")),
            out_specs=(
                P("scan", "ascan", None),
                P("scan", "ascan", None),
                P("scan", "ascan", None),
                P(),
            ),
            check_vma=False,
        )
        return step(spectra, surface_top, surface_bottom)

    return program
```

```python
import functools
import math

import jax
import jax.numpy as jnp
import numpy as np
from jax import lax
from jax.experimental import pallas as pl
from jax.experimental.pallas import tpu as pltpu
from jax.sharding import PartitionSpec as P


REPEATS = 4
BINS = 2048
BANDS = 4
TILE = 128
BAND_BINS = 512
DEPTH = 1024
TILES = DEPTH // TILE
FLOOR = 0.05 * BAND_BINS
VARIANCE_SCALE = 0.1
HEAD = 2
MERGE = 44
UNROLL = 4
MAPS = 3


VMEM = pl.BlockSpec(memory_space=pltpu.VMEM)


def table_values():
    sample = np.arange(BAND_BINS)
    depth = np.arange(DEPTH)
    product = (sample[:, None] * depth[None, :]) % BINS
    angle = product.astype(np.float32) * np.float32(2.0 * math.pi / BINS)
    window = np.sin(np.float32(math.pi) * (sample.astype(np.float32) + 0.5) / BAND_BINS) ** 2
    return window[:, None] * np.cos(angle), window[:, None] * np.sin(angle)


def tile_tables(width):
    cosine, sine = table_values()
    slabs = DEPTH // width
    cosine = cosine.reshape(BAND_BINS, slabs, width)
    sine = sine.reshape(BAND_BINS, slabs, width)
    both = np.concatenate([cosine, sine], axis=2).transpose(1, 0, 2)
    return jnp.asarray(both.astype(np.float32)).astype(jnp.bfloat16)


def moments_rows(profile_ref, buf, out_ref, slot, scan, ascans, begin, end):
    tiny = jnp.float32(np.finfo(np.float32).tiny)
    step = 8
    for start in range(begin, end, step) if isinstance(begin, int) else [pl.multiple_of(begin, step)]:
        sim = amp = var1 = var2 = None
        for band in range(BANDS):
            power, amplitude = [], []
            for repeat in range(REPEATS):
                base = repeat * ascans + start
                re = profile_ref[buf, band, pl.ds(base, step), :TILE]
                im = profile_ref[buf, band, pl.ds(base, step), TILE:]
                p = re * re + im * im
                power.append(p)
                amplitude.append(p * lax.rsqrt(jnp.maximum(p, tiny)))
            parts = []
            for r in range(REPEATS - 1):
                root = lax.rsqrt(jnp.maximum(power[r] + power[r + 1], FLOOR))
                parts.append((amplitude[r] * root) * (amplitude[r + 1] * root))
            s = parts[0] + parts[1] + parts[2]
            s01 = amplitude[0] + amplitude[1]
            s23 = amplitude[2] + amplitude[3]
            d01 = amplitude[0] - amplitude[1]
            d23 = amplitude[2] - amplitude[3]
            a = s01 + s23
            d = s01 - s23
            v1 = d01 * d01 + d23 * d23
            v2 = d * d
            sim = s if sim is None else sim + s
            amp = a if amp is None else amp + a
            var1 = v1 if var1 is None else var1 + v1
            var2 = v2 if var2 is None else var2 + v2
        rows = pl.ds(scan * ascans + start, step)
        out_ref[slot, rows, 0:TILE] = 1.0 - sim * (2.0 / (BANDS * (REPEATS - 1)))
        out_ref[slot, rows, TILE : 2 * TILE] = amp * (1.0 / (BANDS * REPEATS * math.sqrt(BAND_BINS)))
        out_ref[slot, rows, 2 * TILE :] = (var1 + 0.5 * var2) * (
            0.5 / (REPEATS * BANDS * VARIANCE_SCALE * BAND_BINS)
        )


def split(x):
    high = x.astype(jnp.bfloat16)
    low = (x - high.astype(jnp.float32)).astype(jnp.bfloat16)
    return high, low


def tissue(top, bottom, tile):
    rows = top.shape[1]
    mask = jnp.where((top <= tile) & (tile < bottom), 1.0, 0.0).astype(jnp.float32)
    before = lax.broadcasted_iota(jnp.int32, (rows, rows), 0) < lax.broadcasted_iota(
        jnp.int32, (rows, rows), 1
    )
    spread = jnp.broadcast_to(mask, (8, rows)).astype(jnp.bfloat16)
    rank = jnp.dot(spread, before.astype(jnp.bfloat16), preferred_element_type=jnp.float32)[0:1]
    return mask, jnp.where(mask > 0.0, rank, -1.0).astype(jnp.int32)


def chooser(rank, first, count):
    rows = rank.shape[1]
    index = lax.broadcasted_iota(jnp.int32, (count, rows), 0) + first
    return jnp.where(index == rank, 1.0, 0.0).astype(jnp.bfloat16)


def flat_rows(block):
    return jnp.concatenate([block[i : i + 1] for i in range(block.shape[0])], axis=1)


def peer_target(peer, me, half):
    kind, index = peer
    if kind == "far":
        return ((me & half) ^ half) | ((me + index) & (half - 1))
    return me ^ index if kind == "near" else index


def peer_origin(peer, me, half):
    kind, index = peer
    if kind == "far":
        return ((me & half) ^ half) | ((me + half - index) & (half - 1))
    return me ^ index if kind == "near" else index


def send_kernel(peers, messages, rooms, staged, x_ref, table_ref, top_ref, bottom_ref, stats_in, *refs):
    count = sum(len(m) for m in messages)
    outs = refs[:count]
    stats_ref, *rest = refs[count:]
    if staged:
        x_vmem, table_vmem, *rest = rest
    profile_ref, maps_ref, *rest = rest
    slots = len(peers)
    scans, _, ascans, _ = x_ref.shape
    me = lax.axis_index("ascan")
    half = lax.axis_size("ascan") // 2
    tiles = [jnp.asarray(peer_target(p, me, half), jnp.int32) for p in peers]

    def lanes_of(band):
        return slice(band * BAND_BINS, (band + 1) * BAND_BINS)

    if staged:
        x_sem, table_sem = rest

        def x_copy(scan):
            return pltpu.make_async_copy(x_ref.at[scan], x_vmem.at[scan], x_sem.at[scan])

        first = tiles[0]

        def table_copy(index):
            tile = (first + index) & (TILES - 1)
            return pltpu.make_async_copy(
                table_ref.at[tile], table_vmem.at[tile], table_sem.at[index]
            )

        table_copy(0).start()
        for scan in range(scans):
            x_copy(scan).start()
        for index in range(1, TILES):
            table_copy(index).start()
        x_used, table_used = x_vmem, table_vmem
    else:
        x_used, table_used = x_ref, table_ref

    def product(weights, slot, scan, buf, band):
        if staged and slot == 0 and band == 0:
            x_copy(scan).wait()
        x = x_used[scan, :, :, lanes_of(band)].reshape(REPEATS * ascans, BAND_BINS)
        profile_ref[buf, band] = jnp.dot(x, weights, preferred_element_type=jnp.float32)

    def weights_of(slot):
        chosen = tiles[0]
        for i in range(1, slots):
            chosen = jnp.where(slot == i, tiles[i], chosen)
        return table_used[chosen]

    def both(following, current):
        if following:
            if staged and following == (0, 0):
                table_copy(0).wait()
            weights = weights_of(following[0])
        share = ascans // BANDS
        for band in range(BANDS):
            if following:
                product(weights, following[0], following[1], following[1] % 2, band)
            if current:
                moments_rows(
                    profile_ref, current[1] % 2, maps_ref, *current, ascans, band * share, (band + 1) * share
                )

    if slots <= UNROLL:
        order = [(slot, scan) for slot in range(slots) for scan in range(scans)]
        for following, current in zip(order + [None], [None] + order):
            both(following, current)
    else:
        both((0, 0), None)

        def step(slot, carry):
            for scan in range(scans - 1):
                both((slot, scan + 1), (slot, scan))
            both((jnp.minimum(slot + 1, slots - 1), 0), (slot, scans - 1))
            return carry

        lax.fori_loop(0, slots, step, 0)

    if staged:
        for index in range(1, TILES):
            table_copy(index).wait()
    top = flat_rows(top_ref[...])
    bottom = flat_rows(bottom_ref[...])
    rows = top.shape[1]
    flow = jnp.zeros((8, TILE), jnp.float32)
    held = over = jnp.float32(0.0)
    position = 0
    for slot, parts in enumerate(messages):
        mask, rank = tissue(top, bottom, tiles[slot])
        high, low = split(maps_ref[slot])
        spread = jnp.broadcast_to(mask, (8, rows)).astype(jnp.bfloat16)
        flow += jnp.dot(spread, high[:, :TILE], preferred_element_type=jnp.float32)
        flow += jnp.dot(spread, low[:, :TILE], preferred_element_type=jnp.float32)
        count = jnp.sum(mask)
        held += count
        room = jnp.float32(rows)
        for source, value in enumerate(rooms[slot]):
            room = jnp.where(me == source, jnp.float32(value), room)
        over = jnp.where(count > room, 1.0, over)
        for first, size, carried, header in parts:
            out = outs[position]
            position += 1
            choice = chooser(rank, first, size)
            out[...] = jnp.dot(choice, high, preferred_element_type=jnp.float32) + jnp.dot(
                choice, low, preferred_element_type=jnp.float32
            )
            if header:
                out[carried : carried + 1, 0:rows] = top.astype(jnp.float32)
                out[carried + 1 : carried + 2, 0:rows] = bottom.astype(jnp.float32)
    line = lax.broadcasted_iota(jnp.int32, (8, TILE), 0)
    stats_ref[...] = stats_in[...] + jnp.where(
        line == 0, flow, jnp.where(line == 1, held, jnp.where(line == 2, over, 0.0))
    )


def dense_send_kernel(x_ref, table_ref, top_ref, bottom_ref, out_ref, profile_ref, maps_ref):
    scans, _, ascans, _ = x_ref.shape
    top = flat_rows(top_ref[...])
    bottom = flat_rows(bottom_ref[...])
    rows = top.shape[1]

    def step(tile, carry):
        weights = table_ref[tile]

        def scan_step(scan, inner):
            for band in range(BANDS):
                x = x_ref[scan, :, :, band * BAND_BINS : (band + 1) * BAND_BINS]
                profile_ref[0, band] = jnp.dot(
                    x.reshape(REPEATS * ascans, BAND_BINS), weights, preferred_element_type=jnp.float32
                )

            def rows_step(chunk, last):
                moments_rows(profile_ref, 0, maps_ref, 0, scan, ascans, chunk * 8, chunk * 8 + 8)
                return last

            return lax.fori_loop(0, ascans // 8, rows_step, inner)

        lax.fori_loop(0, scans, scan_step, 0)
        high, low = split(maps_ref[0])
        mask = (top <= tile) & (tile < bottom)
        same = lax.broadcasted_iota(jnp.int32, (rows, rows), 0) == lax.broadcasted_iota(
            jnp.int32, (rows, rows), 1
        )
        choice = jnp.where(same & mask, 1.0, 0.0).astype(jnp.bfloat16)
        out_ref[tile] = jnp.dot(choice, high, preferred_element_type=jnp.float32) + jnp.dot(
            choice, low, preferred_element_type=jnp.float32
        )
        return carry

    lax.fori_loop(0, TILES, step, 0)


def dense_send(spectra, tables, top, bottom):
    scans, repeats, ascans, _ = spectra.shape
    rows = scans * ascans
    return pl.pallas_call(
        dense_send_kernel,
        out_shape=jax.ShapeDtypeStruct((TILES, rows, MAPS * TILE), jnp.float32),
        in_specs=[VMEM] * 4,
        out_specs=VMEM,
        scratch_shapes=[
            pltpu.VMEM((1, BANDS, repeats * ascans, 2 * TILE), jnp.float32),
            pltpu.VMEM((1, rows, MAPS * TILE), jnp.float32),
        ],
        compiler_params=pltpu.CompilerParams(vmem_limit_bytes=32 * 1024 * 1024),
        name="dense_send",
    )(spectra, tables, top, bottom)


def send(peers, spectra, tables, top, bottom, stats, messages, rooms, staged=False):
    scans, repeats, ascans, bins = spectra.shape
    assert scans % 2 == 0
    rows = scans * ascans
    shapes = [
        jax.ShapeDtypeStruct((size, MAPS * TILE), jnp.float32)
        for parts in messages
        for _, size, _, _ in parts
    ]
    shapes.append(jax.ShapeDtypeStruct((8, TILE), jnp.float32))
    if staged:
        assert len(peers) == 1
        shapes.append(jax.ShapeDtypeStruct(spectra.shape, spectra.dtype))
        shapes.append(jax.ShapeDtypeStruct(tables.shape, tables.dtype))
    scratch = [
        pltpu.VMEM((2, BANDS, repeats * ascans, 2 * TILE), jnp.float32),
        pltpu.VMEM((len(peers), rows, MAPS * TILE), jnp.float32),
    ]
    specs = [VMEM] * 5
    if staged:
        scratch += [
            pltpu.SemaphoreType.DMA((scans,)),
            pltpu.SemaphoreType.DMA((TILES,)),
        ]
        specs[:2] = [pl.BlockSpec(memory_space=pltpu.HBM)] * 2
    return pl.pallas_call(
        functools.partial(send_kernel, peers, messages, rooms, staged),
        out_shape=shapes,
        in_specs=specs,
        out_specs=[VMEM] * len(shapes),
        scratch_shapes=scratch,
        cost_estimate=pl.CostEstimate(
            flops=2 * rows * repeats * bins * 2 * TILE * len(peers),
            bytes_accessed=2 * spectra.size,
            transcendentals=0,
        ),
        compiler_params=pltpu.CompilerParams(vmem_limit_bytes=18 * 1024 * 1024),
    )(spectra, tables, top, bottom, stats)


def mean_scale(totals):
    flow = jnp.sum(totals[0:1, :], axis=1, keepdims=True)
    return (totals[1:2, 0:1] * TILE) / (3.0 * flow)


def smooth(decorrelation_ref, angiogram_ref, scale):
    scans, _, total = angiogram_ref.shape
    step = 8
    for scan in range(scans):
        for start in range(0, TILE, step):
            d = decorrelation_ref[scan, start : start + step, :]
            lane = lax.broadcasted_iota(jnp.int32, d.shape, 1)
            left = jnp.where(lane == 0, 0.0, pltpu.roll(d, 1, 1))
            right = jnp.where(lane == total - 1, 0.0, pltpu.roll(d, total - 1, 1))
            angiogram_ref[scan, start : start + step, :] = ((left + d) + right) * scale


def place(piece, choice):
    result = None
    for part in split(piece):
        term = lax.dot_general(
            part, choice, (((0,), (0,)), ((), ())), preferred_element_type=jnp.float32
        )
        result = term if result is None else result + term
    return result


def receive_kernel(peers, messages, totals_ref, top_ref, bottom_ref, *refs):
    count = sum(len(m) for m in messages)
    ins = refs[:count]
    angiogram_ref, structure_ref, speckle_ref, decorrelation_ref = refs[count:]
    scans = angiogram_ref.shape[0]
    own_top = flat_rows(top_ref[...])
    own_bottom = flat_rows(bottom_ref[...])
    rows = own_top.shape[1]
    ascans = rows // scans
    me = lax.axis_index("ascan")
    half = lax.axis_size("ascan") // 2
    position = 0
    for peer, parts in zip(peers, messages):
        pieces = ins[position : position + len(parts)]
        position += len(parts)
        top, bottom = own_top, own_bottom
        for piece, (_, _, carried, header) in zip(pieces, parts):
            if header:
                top = piece[carried : carried + 1, 0:rows].astype(jnp.int32)
                bottom = piece[carried + 1 : carried + 2, 0:rows].astype(jnp.int32)
        _, rank = tissue(top, bottom, me)
        result = None
        for piece, (first, size, carried, header) in zip(pieces, parts):
            choice = chooser(jnp.where(rank < first + carried, rank, -1), first, size)
            term = place(piece[...], choice)
            result = term if result is None else result + term
        origin = jnp.asarray(peer_origin(peer, me, half), jnp.int32)
        lanes = pl.ds(pl.multiple_of(origin * ascans, ascans), ascans)
        for scan in range(scans):
            columns = slice(scan * ascans, (scan + 1) * ascans)
            decorrelation_ref[scan, :, lanes] = result[0:TILE, columns]
            structure_ref[scan, :, lanes] = result[TILE : 2 * TILE, columns]
            speckle_ref[scan, :, lanes] = result[2 * TILE :, columns]
    smooth(decorrelation_ref, angiogram_ref, mean_scale(totals_ref[...]))


def dense_receive_kernel(totals_ref, pieces_ref, angiogram_ref, structure_ref, speckle_ref, decorrelation_ref):
    members, rows, _ = pieces_ref.shape
    scans = angiogram_ref.shape[0]
    ascans = rows // scans
    same = lax.broadcasted_iota(jnp.int32, (rows, rows), 0) == lax.broadcasted_iota(
        jnp.int32, (rows, rows), 1
    )
    choice = jnp.where(same, 1.0, 0.0).astype(jnp.bfloat16)

    def step(source, carry):
        result = place(pieces_ref[source], choice)
        lanes = pl.ds(pl.multiple_of(source * ascans, ascans), ascans)
        for scan in range(scans):
            columns = slice(scan * ascans, (scan + 1) * ascans)
            decorrelation_ref[scan, :, lanes] = result[0:TILE, columns]
            structure_ref[scan, :, lanes] = result[TILE : 2 * TILE, columns]
            speckle_ref[scan, :, lanes] = result[2 * TILE :, columns]
        return carry

    lax.fori_loop(0, members, step, 0)
    smooth(decorrelation_ref, angiogram_ref, mean_scale(totals_ref[...]))


def result_call(kernel, operands, scans, total):
    shape = jax.ShapeDtypeStruct((scans, TILE, total), jnp.float32)
    return tuple(
        pl.pallas_call(
            kernel,
            out_shape=[shape] * MAPS,
            in_specs=[VMEM] * len(operands),
            out_specs=[VMEM] * MAPS,
            scratch_shapes=[pltpu.VMEM(shape.shape, jnp.float32)],
            cost_estimate=pl.CostEstimate(
                flops=1024 * scans * MAPS * TILE * total,
                bytes_accessed=8 * MAPS * scans * TILE * total,
                transcendentals=0,
            ),
            compiler_params=pltpu.CompilerParams(vmem_limit_bytes=24 * 1024 * 1024),
        )(*operands)
    )


def capacities(members, scans, ascans):
    total = members * ascans
    position = np.arange(total)
    chance = np.zeros((total, TILES))
    half = TILES // 2
    for top in range(half):
        reach = 1 + (TILES - top - 1) * (position + 1) // total
        for tile in range(top, TILES):
            chance[:, tile] += np.clip(reach - (tile - top), 0, None) / reach / half
    mean = chance.reshape(members, ascans, TILES).sum(1) * scans
    spread = np.sqrt((chance * (1 - chance)).reshape(members, ascans, TILES).sum(1) * scans)
    caps = np.ceil(mean + 3.8 * spread)
    return np.minimum(caps, scans * ascans).astype(int)


def plan_levels(caps, matching, merge):
    need = [int(caps[s, d]) + (HEAD if s != d else 0) for s, d in matching]
    base = -(-sorted(need)[len(need) // 2] // 8) * 8
    need = [max(n, base) for n in need]
    marks = []
    for value in sorted(set(-(-n // 8) * 8 for n in need), reverse=True):
        if not marks or value == base or marks[0] - value >= merge:
            marks.insert(0, value)
    messages, pair_lists, room, below = [], [], [0] * len(need), 0
    for mark in marks:
        pairs = [pair for pair, n in zip(matching, need) if n > below]
        head = HEAD if below == 0 else 0
        for s, _ in pairs:
            room[s] = mark - HEAD
        first = max(below - HEAD, 0)
        messages.append((first, mark - below, mark - below - head, head > 0))
        pair_lists.append(pairs)
        below = mark
    return tuple(messages), pair_lists, tuple(room)


def exchange_plans(members, scans, ascans):
    rows = scans * ascans
    half = members // 2
    caps = capacities(members, scans, ascans)
    far = [("far", m) for m in range(half)]
    near = [("near", j) for j in range(1, half)]
    own = ("near", 0)

    def pairs_of(peer):
        return [(s, int(peer_target(peer, s, half))) for s in range(members)]

    plans = {peer: plan_levels(caps, pairs_of(peer), MERGE) for peer in far}
    widest = max(int(caps[s, d]) for peer in near for s, d in pairs_of(peer))
    head = HEAD
    size = -(-(widest + head) // 8) * 8
    for peer in near:
        plans[peer] = (
            ((0, size, size - head, True),),
            [pairs_of(peer)],
            (size - head,) * members,
        )
    plans[own] = (((0, rows, rows, False),), [None], (rows,) * members)
    return plans, far, near, own


def sparse_body(members, spectra, top, bottom):
    scans, _, ascans, _ = spectra.shape
    tables = tile_tables(TILE)
    plans, far, near, own = exchange_plans(members, scans, ascans)
    stats = jnp.zeros((8, TILE), jnp.float32)
    sent = {}
    spectra_here, tables_here = spectra, tables
    peers = far + near + [own]
    for number, group in enumerate(tile_groups(far, near, own)):
        out = list(
            send(
                group,
                spectra_here,
                tables_here,
                top,
                bottom,
                stats,
                [plans[p][0] for p in group],
                [plans[p][2] for p in group],
                staged=number == 0,
            )
        )
        for peer in group:
            for level in range(len(plans[peer][0])):
                sent[peer, level] = out.pop(0)
        stats = out.pop(0)
        if number == 0:
            spectra_here, tables_here = out
    length = lax.axis_size("scan")
    hops = [("ascan", flipped(members, 1))]
    hops += [("scan", flipped(length, stride)) for stride in strides(length)]
    for axis, pairs in hops:
        stats = stats + lax.ppermute(stats, axis, pairs)
    received, shares = [], [stats]
    for peer in peers:
        for level, pairs in enumerate(plans[peer][1]):
            message = sent[peer, level]
            if pairs is not None:
                message = lax.ppermute(message, "ascan", pairs)
            received.append(message)
    for bits in range(2, members, 2):
        shares.append(lax.ppermute(stats, "ascan", flipped(members, bits)))
    totals = functools.reduce(jnp.add, shares)
    mean_flow = jnp.sum(totals[0]) / (totals[1, 0] * TILE)

    def quick(received):
        kernel = functools.partial(receive_kernel, peers, [plans[p][0] for p in peers])
        return result_call(kernel, [totals, top, bottom, *received], scans, members * ascans)

    def dense(received):
        out = dense_send(spectra, tables, top, bottom)
        swapped = lax.all_to_all(out, "ascan", 0, 0, tiled=True)
        return result_call(dense_receive_kernel, [totals, swapped], scans, members * ascans)

    outs = lax.cond(totals[2, 0] > 0.0, dense, quick, received)
    return (*outs, mean_flow)


def flipped(length, bits):
    return [(s, s ^ bits) for s in range(length)]


def strides(length):
    return [1 << bit for bit in range(length.bit_length() - 1)]


def tile_groups(far, near, own):
    return far[:1], far[1:2], far[2:], near + [own]


def plain_body(spectra, surface_top, surface_bottom):
    scans, repeats, ascans, _ = spectra.shape
    cosine, sine = table_values()
    table = jnp.asarray(np.concatenate([cosine, sine], axis=1).astype(np.float32)).astype(jnp.bfloat16)
    similarity = amplitude_sum = variance = jnp.zeros((scans, ascans, DEPTH), jnp.float32)
    for band in range(BANDS):
        part = spectra[..., band * BAND_BINS : (band + 1) * BAND_BINS]
        profile = jnp.dot(part.reshape(-1, BAND_BINS), table, preferred_element_type=jnp.float32)
        profile = profile.reshape(scans, repeats, ascans, 2 * DEPTH)
        amplitude = jnp.sqrt(profile[..., :DEPTH] ** 2 + profile[..., DEPTH:] ** 2)
        first, second = amplitude[:, :-1], amplitude[:, 1:]
        similarity += jnp.sum(
            2.0 * first * second / jnp.maximum(first**2 + second**2, FLOOR), axis=1
        )
        amplitude_sum += jnp.sum(amplitude, axis=1)
        center = jnp.mean(amplitude, axis=1, keepdims=True)
        variance += jnp.mean((amplitude - center) ** 2, axis=1)
    depth = jnp.arange(DEPTH, dtype=jnp.int32)
    inside = (depth >= surface_top[..., None] * TILE) & (depth < surface_bottom[..., None] * TILE)
    inside = inside.astype(jnp.float32)
    decorrelation = (1.0 - similarity / (BANDS * (REPEATS - 1))) * inside
    structure = amplitude_sum / (BANDS * REPEATS) / math.sqrt(BAND_BINS) * inside
    speckle = variance / BANDS / (VARIANCE_SCALE * BAND_BINS) * inside
    totals = lax.psum((jnp.sum(decorrelation), jnp.sum(inside)), ("scan", "ascan"))
    mean_flow = totals[0] / totals[1]
    decorrelation, structure, speckle = (
        lax.all_to_all(x, "ascan", split_axis=2, concat_axis=1, tiled=True)
        for x in (decorrelation, structure, speckle)
    )
    padded = jnp.pad(decorrelation, ((0, 0), (1, 1), (0, 0)))
    smoothed = (padded[:, :-2] + padded[:, 1:-1] + padded[:, 2:]) / 3.0
    angiogram = jnp.swapaxes(smoothed / mean_flow, 1, 2)
    return (angiogram, jnp.swapaxes(structure, 1, 2), jnp.swapaxes(speckle, 1, 2), mean_flow)


def solution(mesh):
    members = mesh.shape["ascan"]
    scans = mesh.shape["scan"]

    def fits(spectra):
        local_scans, ascans = spectra.shape[0] // scans, spectra.shape[2] // members
        return (
            members == TILES
            and scans & (scans - 1) == 0
            and local_scans % 2 == 0
            and ascans == TILE
            and local_scans * ascans <= MAPS * TILE
        )

    def program(spectra, surface_top, surface_bottom):
        sparse = fits(spectra)
        body = functools.partial(sparse_body, members) if sparse else plain_body
        step = jax.shard_map(
            body,
            mesh=mesh,
            in_specs=(P("scan", None, "ascan", None), P("scan", "ascan"), P("scan", "ascan")),
            out_specs=(
                P("scan", "ascan", None),
                P("scan", "ascan", None),
                P("scan", "ascan", None),
                P(),
            ),
            check_vma=False,
        )
        return step(spectra, surface_top, surface_bottom)

    return program
```

```python
import functools
import math

import jax
import jax.numpy as jnp
import numpy as np
from jax import lax
from jax.experimental import pallas as pl
from jax.experimental.pallas import tpu as pltpu
from jax.sharding import PartitionSpec as P


REPEATS = 4
BINS = 2048
BANDS = 4
TILE = 128
BAND_BINS = 512
DEPTH = 1024
TILES = DEPTH // TILE
FLOOR = 0.05 * BAND_BINS
VARIANCE_SCALE = 0.1
HEAD = 2
MERGE = 44
MAPS = 3


VMEM = pl.BlockSpec(memory_space=pltpu.VMEM)


def table_values():
    sample = np.arange(BAND_BINS)
    depth = np.arange(DEPTH)
    product = (sample[:, None] * depth[None, :]) % BINS
    angle = product.astype(np.float32) * np.float32(2.0 * math.pi / BINS)
    window = np.sin(np.float32(math.pi) * (sample.astype(np.float32) + 0.5) / BAND_BINS) ** 2
    return window[:, None] * np.cos(angle), window[:, None] * np.sin(angle)


def tile_tables(width):
    cosine, sine = table_values()
    slabs = DEPTH // width
    cosine = cosine.reshape(BAND_BINS, slabs, width)
    sine = sine.reshape(BAND_BINS, slabs, width)
    both = np.concatenate([cosine, sine], axis=2).transpose(1, 0, 2)
    return jnp.asarray(both.astype(np.float32)).astype(jnp.bfloat16)


def moments_rows(profile_ref, buf, out_ref, slot, scan, ascans, begin, end):
    tiny = jnp.float32(np.finfo(np.float32).tiny)
    step = 8
    for start in range(begin, end, step) if isinstance(begin, int) else [pl.multiple_of(begin, step)]:
        sim = amp = var1 = var2 = None
        for band in range(BANDS):
            power, amplitude = [], []
            for repeat in range(REPEATS):
                base = repeat * ascans + start
                re = profile_ref[buf, band, pl.ds(base, step), :TILE]
                im = profile_ref[buf, band, pl.ds(base, step), TILE:]
                p = re * re + im * im
                power.append(p)
                amplitude.append(p * lax.rsqrt(jnp.maximum(p, tiny)))
            parts = []
            for r in range(REPEATS - 1):
                root = lax.rsqrt(jnp.maximum(power[r] + power[r + 1], FLOOR))
                parts.append((amplitude[r] * root) * (amplitude[r + 1] * root))
            s = parts[0] + parts[1] + parts[2]
            s01 = amplitude[0] + amplitude[1]
            s23 = amplitude[2] + amplitude[3]
            d01 = amplitude[0] - amplitude[1]
            d23 = amplitude[2] - amplitude[3]
            a = s01 + s23
            d = s01 - s23
            v1 = d01 * d01 + d23 * d23
            v2 = d * d
            sim = s if sim is None else sim + s
            amp = a if amp is None else amp + a
            var1 = v1 if var1 is None else var1 + v1
            var2 = v2 if var2 is None else var2 + v2
        rows = pl.ds(scan * ascans + start, step)
        out_ref[slot, rows, 0:TILE] = 1.0 - sim * (2.0 / (BANDS * (REPEATS - 1)))
        out_ref[slot, rows, TILE : 2 * TILE] = amp * (1.0 / (BANDS * REPEATS * math.sqrt(BAND_BINS)))
        out_ref[slot, rows, 2 * TILE :] = (var1 + 0.5 * var2) * (
            0.5 / (REPEATS * BANDS * VARIANCE_SCALE * BAND_BINS)
        )


def split(x):
    high = x.astype(jnp.bfloat16)
    low = (x - high.astype(jnp.float32)).astype(jnp.bfloat16)
    return high, low


def tissue(top, bottom, tile):
    rows = top.shape[1]
    mask = jnp.where((top <= tile) & (tile < bottom), 1.0, 0.0).astype(jnp.float32)
    before = lax.broadcasted_iota(jnp.int32, (rows, rows), 0) < lax.broadcasted_iota(
        jnp.int32, (rows, rows), 1
    )
    spread = jnp.broadcast_to(mask, (8, rows)).astype(jnp.bfloat16)
    rank = jnp.dot(spread, before.astype(jnp.bfloat16), preferred_element_type=jnp.float32)[0:1]
    return mask, jnp.where(mask > 0.0, rank, -1.0).astype(jnp.int32)


def chooser(rank, first, count):
    rows = rank.shape[1]
    index = lax.broadcasted_iota(jnp.int32, (count, rows), 0) + first
    return jnp.where(index == rank, 1.0, 0.0).astype(jnp.bfloat16)


def flat_rows(block):
    return jnp.concatenate([block[i : i + 1] for i in range(block.shape[0])], axis=1)


def peer_target(peer, me, half):
    kind, index = peer
    if kind == "far":
        return ((me & half) ^ half) | ((me + index) & (half - 1))
    return me ^ index if kind == "near" else index


def peer_origin(peer, me, half):
    kind, index = peer
    if kind == "far":
        return ((me & half) ^ half) | ((me + half - index) & (half - 1))
    return me ^ index if kind == "near" else index


def send_kernel(peers, messages, x_ref, table_ref, top_ref, bottom_ref, stats_in, *refs):
    count = sum(len(m) for m in messages)
    outs = refs[:count]
    stats_ref, *rest = refs[count:]
    profile_ref, maps_ref = rest
    slots = len(peers)
    scans, _, ascans, _ = x_ref.shape
    me = lax.axis_index("ascan")
    half = lax.axis_size("ascan") // 2
    tiles = [jnp.asarray(peer_target(p, me, half), jnp.int32) for p in peers]

    def lanes_of(band):
        return slice(band * BAND_BINS, (band + 1) * BAND_BINS)

    def product(weights, scan, buf, band):
        x = x_ref[scan, :, :, lanes_of(band)].reshape(REPEATS * ascans, BAND_BINS)
        profile_ref[buf, band] = jnp.dot(x, weights, preferred_element_type=jnp.float32)

    def weights_of(slot):
        return table_ref[tiles[slot]]

    def both(following, current):
        if following:
            weights = weights_of(following[0])
        share = ascans // BANDS
        for band in range(BANDS):
            if following:
                product(weights, following[1], following[1] % 2, band)
            if current:
                moments_rows(
                    profile_ref, current[1] % 2, maps_ref, *current, ascans, band * share, (band + 1) * share
                )

    top = flat_rows(top_ref[...])
    bottom = flat_rows(bottom_ref[...])
    rows = top.shape[1]
    full = [
        jnp.sum(jnp.where((top <= tile) & (tile < bottom), 1.0, 0.0)) > 0.0 for tile in tiles
    ]
    every = functools.reduce(jnp.logical_and, full)

    @pl.when(every)
    def _():
        order = [(slot, scan) for slot in range(slots) for scan in range(scans)]
        for following, current in zip(order + [None], [None] + order):
            both(following, current)

    for slot in range(slots):

        @pl.when(jnp.logical_not(full[slot]))
        def _():
            maps_ref[slot] = jnp.zeros(maps_ref.shape[1:], jnp.float32)

        if slots > 1:

            @pl.when(full[slot] & jnp.logical_not(every))
            def _():
                both((slot, 0), None)
                for scan in range(scans - 1):
                    both((slot, scan + 1), (slot, scan))
                both(None, (slot, scans - 1))

    flow = jnp.zeros((8, TILE), jnp.float32)
    held = jnp.float32(0.0)
    position = 0
    for slot, parts in enumerate(messages):
        mask, rank = tissue(top, bottom, tiles[slot])
        high, low = split(maps_ref[slot])
        spread = jnp.broadcast_to(mask, (8, rows)).astype(jnp.bfloat16)
        flow += jnp.dot(spread, high[:, :TILE], preferred_element_type=jnp.float32)
        flow += jnp.dot(spread, low[:, :TILE], preferred_element_type=jnp.float32)
        count = jnp.sum(mask)
        held += count
        for first, size, carried, header in parts:
            out = outs[position]
            position += 1
            choice = chooser(rank, first, size)
            out[...] = jnp.dot(choice, high, preferred_element_type=jnp.float32) + jnp.dot(
                choice, low, preferred_element_type=jnp.float32
            )
            if header:
                out[carried : carried + 1, 0:rows] = top.astype(jnp.float32)
                out[carried + 1 : carried + 2, 0:rows] = bottom.astype(jnp.float32)
    line = lax.broadcasted_iota(jnp.int32, (8, TILE), 0)
    stats_ref[...] = stats_in[...] + jnp.where(
        line == 0, flow, jnp.where(line == 1, held, 0.0)
    )


def dense_send_kernel(x_ref, table_ref, top_ref, bottom_ref, out_ref, profile_ref, maps_ref):
    scans, _, ascans, _ = x_ref.shape
    top = flat_rows(top_ref[...])
    bottom = flat_rows(bottom_ref[...])
    rows = top.shape[1]

    def step(tile, carry):
        weights = table_ref[tile]

        def scan_step(scan, inner):
            for band in range(BANDS):
                x = x_ref[scan, :, :, band * BAND_BINS : (band + 1) * BAND_BINS]
                profile_ref[0, band] = jnp.dot(
                    x.reshape(REPEATS * ascans, BAND_BINS), weights, preferred_element_type=jnp.float32
                )

            def rows_step(chunk, last):
                moments_rows(profile_ref, 0, maps_ref, 0, scan, ascans, chunk * 8, chunk * 8 + 8)
                return last

            return lax.fori_loop(0, ascans // 8, rows_step, inner)

        lax.fori_loop(0, scans, scan_step, 0)
        high, low = split(maps_ref[0])
        mask = (top <= tile) & (tile < bottom)
        same = lax.broadcasted_iota(jnp.int32, (rows, rows), 0) == lax.broadcasted_iota(
            jnp.int32, (rows, rows), 1
        )
        choice = jnp.where(same & mask, 1.0, 0.0).astype(jnp.bfloat16)
        out_ref[tile] = jnp.dot(choice, high, preferred_element_type=jnp.float32) + jnp.dot(
            choice, low, preferred_element_type=jnp.float32
        )
        return carry

    lax.fori_loop(0, TILES, step, 0)


def dense_send(spectra, tables, top, bottom):
    scans, repeats, ascans, _ = spectra.shape
    rows = scans * ascans
    return pl.pallas_call(
        dense_send_kernel,
        out_shape=jax.ShapeDtypeStruct((TILES, rows, MAPS * TILE), jnp.float32),
        in_specs=[VMEM] * 4,
        out_specs=VMEM,
        scratch_shapes=[
            pltpu.VMEM((1, BANDS, repeats * ascans, 2 * TILE), jnp.float32),
            pltpu.VMEM((1, rows, MAPS * TILE), jnp.float32),
        ],
        compiler_params=pltpu.CompilerParams(vmem_limit_bytes=20 * 1024 * 1024),
        name="dense_send",
    )(spectra, tables, top, bottom)


def send(peers, spectra, tables, top, bottom, stats, messages):
    scans, repeats, ascans, bins = spectra.shape
    assert scans % 2 == 0
    rows = scans * ascans
    shapes = [
        jax.ShapeDtypeStruct((size, MAPS * TILE), jnp.float32)
        for parts in messages
        for _, size, _, _ in parts
    ]
    shapes.append(jax.ShapeDtypeStruct((8, TILE), jnp.float32))
    scratch = [
        pltpu.VMEM((2, BANDS, repeats * ascans, 2 * TILE), jnp.float32),
        pltpu.VMEM((len(peers), rows, MAPS * TILE), jnp.float32),
    ]
    specs = [VMEM] * 5
    return pl.pallas_call(
        functools.partial(send_kernel, peers, messages),
        out_shape=shapes,
        in_specs=specs,
        out_specs=[VMEM] * len(shapes),
        scratch_shapes=scratch,
        cost_estimate=pl.CostEstimate(
            flops=2 * rows * repeats * bins * 2 * TILE * len(peers),
            bytes_accessed=2 * spectra.size,
            transcendentals=0,
        ),
        compiler_params=pltpu.CompilerParams(vmem_limit_bytes=18 * 1024 * 1024),
    )(spectra, tables, top, bottom, stats)


def mean_of(shares):
    values = [share[...] for share in shares]
    while len(values) > 1:
        values = [a + b for a, b in zip(values[::2], values[1::2])]
    flow = jnp.sum(values[0][0:1, :], axis=1, keepdims=True)
    return flow / (values[0][1:2, 0:1] * TILE)


def smooth(decorrelation_ref, angiogram_ref, scale):
    scans, _, total = angiogram_ref.shape
    step = 8
    for scan in range(scans):
        for start in range(0, TILE, step):
            d = decorrelation_ref[scan, start : start + step, :]
            lane = lax.broadcasted_iota(jnp.int32, d.shape, 1)
            left = jnp.where(lane == 0, 0.0, pltpu.roll(d, 1, 1))
            right = jnp.where(lane == total - 1, 0.0, pltpu.roll(d, total - 1, 1))
            added = (left + d) + right
            angiogram_ref[scan, start : start + step, :] = added if scale is None else added * scale


def place(piece, choice):
    result = None
    for part in split(piece):
        term = lax.dot_general(
            part, choice, (((0,), (0,)), ((), ())), preferred_element_type=jnp.float32
        )
        result = term if result is None else result + term
    return result


def receive_kernel(peers, messages, top_ref, bottom_ref, *refs):
    count = sum(len(m) for m in messages)
    ins = refs[:count]
    angiogram_ref, structure_ref, speckle_ref, decorrelation_ref = refs[count:]
    scans = angiogram_ref.shape[0]
    own_top = flat_rows(top_ref[...])
    own_bottom = flat_rows(bottom_ref[...])
    rows = own_top.shape[1]
    ascans = rows // scans
    me = lax.axis_index("ascan")
    half = lax.axis_size("ascan") // 2
    position = 0
    for peer, parts in zip(peers, messages):
        pieces = ins[position : position + len(parts)]
        position += len(parts)
        top, bottom = own_top, own_bottom
        for piece, (_, _, carried, header) in zip(pieces, parts):
            if header:
                top = piece[carried : carried + 1, 0:rows].astype(jnp.int32)
                bottom = piece[carried + 1 : carried + 2, 0:rows].astype(jnp.int32)
        _, rank = tissue(top, bottom, me)
        result = None
        for piece, (first, size, carried, header) in zip(pieces, parts):
            choice = chooser(jnp.where(rank < first + carried, rank, -1), first, size)
            term = place(piece[...], choice)
            result = term if result is None else result + term
        origin = jnp.asarray(peer_origin(peer, me, half), jnp.int32)
        lanes = pl.ds(pl.multiple_of(origin * ascans, ascans), ascans)
        for scan in range(scans):
            columns = slice(scan * ascans, (scan + 1) * ascans)
            decorrelation_ref[scan, :, lanes] = result[0:TILE, columns]
            structure_ref[scan, :, lanes] = result[TILE : 2 * TILE, columns]
            speckle_ref[scan, :, lanes] = result[2 * TILE :, columns]
    smooth(decorrelation_ref, angiogram_ref, None)


def finish_kernel(count, sums_ref, *refs):
    shares, (angiogram_ref, mean_ref) = refs[:count], refs[count:]
    mean = mean_of(shares)
    mean_ref[...] = jnp.broadcast_to(mean, mean_ref.shape)
    angiogram_ref[...] = sums_ref[...] * (1.0 / (3.0 * mean))


def finish(sums, shares):
    return pl.pallas_call(
        functools.partial(finish_kernel, len(shares)),
        out_shape=[
            jax.ShapeDtypeStruct(sums.shape, jnp.float32),
            jax.ShapeDtypeStruct((8, TILE), jnp.float32),
        ],
        in_specs=[VMEM] * (1 + len(shares)),
        out_specs=[VMEM, VMEM],
        compiler_params=pltpu.CompilerParams(vmem_limit_bytes=8 * 1024 * 1024),
        name="finish_angiogram",
    )(sums, *shares)


def judge_kernel(peers, carried, room_ref, top_ref, bottom_ref, *refs):
    pieces, out_ref = refs[:-1], refs[-1]
    me = lax.axis_index("ascan")
    half = lax.axis_size("ascan") // 2
    own_top = flat_rows(top_ref[...]).astype(jnp.float32)
    own_bottom = flat_rows(bottom_ref[...]).astype(jnp.float32)
    rows = own_top.shape[1]
    tile = lax.broadcasted_iota(jnp.int32, (TILES, rows), 0).astype(jnp.float32)
    worst = jnp.full((TILES, 1), -1.0, jnp.float32)
    surfaces = [(me, own_top, own_bottom)]
    for peer, piece, line in zip(peers, pieces, carried):
        origin = jnp.asarray(peer_origin(peer, me, half), jnp.int32)
        surfaces.append((origin, piece[line : line + 1, 0:rows], piece[line + 1 : line + 2, 0:rows]))
    for source, top, bottom in surfaces:
        need = jnp.sum(jnp.where((top <= tile) & (tile < bottom), 1.0, 0.0), axis=1, keepdims=True)
        worst = jnp.maximum(worst, need - room_ref[source][:, 0:1])
    out_ref[0, 0] = jnp.where(jnp.max(worst) > 0.0, 1, 0).astype(jnp.int32)


def judge(peers, carried, room, top, bottom, pieces):
    return pl.pallas_call(
        functools.partial(judge_kernel, peers, carried),
        out_shape=jax.ShapeDtypeStruct((1, 1), jnp.int32),
        in_specs=[VMEM] * (3 + len(pieces)),
        out_specs=pl.BlockSpec(memory_space=pltpu.SMEM),
        compiler_params=pltpu.CompilerParams(vmem_limit_bytes=8 * 1024 * 1024),
        name="judge_room",
    )(room, top, bottom, *pieces)


def dense_receive_kernel(pieces_ref, *refs):
    shares = refs[:-5]
    angiogram_ref, structure_ref, speckle_ref, mean_ref, decorrelation_ref = refs[-5:]
    members, rows, _ = pieces_ref.shape
    scans = angiogram_ref.shape[0]
    ascans = rows // scans
    same = lax.broadcasted_iota(jnp.int32, (rows, rows), 0) == lax.broadcasted_iota(
        jnp.int32, (rows, rows), 1
    )
    choice = jnp.where(same, 1.0, 0.0).astype(jnp.bfloat16)

    def step(source, carry):
        result = place(pieces_ref[source], choice)
        lanes = pl.ds(pl.multiple_of(source * ascans, ascans), ascans)
        for scan in range(scans):
            columns = slice(scan * ascans, (scan + 1) * ascans)
            decorrelation_ref[scan, :, lanes] = result[0:TILE, columns]
            structure_ref[scan, :, lanes] = result[TILE : 2 * TILE, columns]
            speckle_ref[scan, :, lanes] = result[2 * TILE :, columns]
        return carry

    lax.fori_loop(0, members, step, 0)
    mean = mean_of(shares)
    mean_ref[...] = jnp.broadcast_to(mean, mean_ref.shape)
    smooth(decorrelation_ref, angiogram_ref, 1.0 / (3.0 * mean))


def result_call(kernel, operands, scans, total, extra=()):
    shape = jax.ShapeDtypeStruct((scans, TILE, total), jnp.float32)
    return tuple(
        pl.pallas_call(
            kernel,
            out_shape=[shape] * MAPS + list(extra),
            in_specs=[VMEM] * len(operands),
            out_specs=[VMEM] * (MAPS + len(extra)),
            scratch_shapes=[pltpu.VMEM(shape.shape, jnp.float32)],
            cost_estimate=pl.CostEstimate(
                flops=1024 * scans * MAPS * TILE * total,
                bytes_accessed=8 * MAPS * scans * TILE * total,
                transcendentals=0,
            ),
            compiler_params=pltpu.CompilerParams(vmem_limit_bytes=16 * 1024 * 1024),
        )(*operands)
    )


def capacities(members, scans, ascans):
    total = members * ascans
    position = np.arange(total)
    chance = np.zeros((total, TILES))
    half = TILES // 2
    for top in range(half):
        reach = 1 + (TILES - top - 1) * (position + 1) // total
        for tile in range(top, TILES):
            chance[:, tile] += np.clip(reach - (tile - top), 0, None) / reach / half
    mean = chance.reshape(members, ascans, TILES).sum(1) * scans
    spread = np.sqrt((chance * (1 - chance)).reshape(members, ascans, TILES).sum(1) * scans)
    caps = np.ceil(mean + 3.8 * spread)
    return np.minimum(caps, scans * ascans).astype(int)


def plan_levels(caps, matching, merge):
    need = [int(caps[s, d]) + (HEAD if s != d else 0) for s, d in matching]
    base = -(-sorted(need)[len(need) // 2] // 8) * 8
    need = [max(n, base) for n in need]
    marks = []
    for value in sorted(set(-(-n // 8) * 8 for n in need), reverse=True):
        if not marks or value == base or marks[0] - value >= merge:
            marks.insert(0, value)
    messages, pair_lists, room, below = [], [], [0] * len(need), 0
    for mark in marks:
        pairs = [pair for pair, n in zip(matching, need) if n > below]
        head = HEAD if below == 0 else 0
        for s, _ in pairs:
            room[s] = mark - HEAD
        first = max(below - HEAD, 0)
        messages.append((first, mark - below, mark - below - head, head > 0))
        pair_lists.append(pairs)
        below = mark
    return tuple(messages), pair_lists, tuple(room)


def exchange_plans(members, scans, ascans):
    rows = scans * ascans
    half = members // 2
    caps = capacities(members, scans, ascans)
    far = [("far", m) for m in range(half)]
    near = [("near", j) for j in range(1, half)]
    own = ("near", 0)

    def pairs_of(peer):
        return [(s, int(peer_target(peer, s, half))) for s in range(members)]

    plans = {peer: plan_levels(caps, pairs_of(peer), MERGE) for peer in far}
    widest = max(int(caps[s, d]) for peer in near for s, d in pairs_of(peer))
    head = HEAD
    size = -(-(widest + head) // 8) * 8
    for peer in near:
        plans[peer] = (
            ((0, size, size - head, True),),
            [pairs_of(peer)],
            (size - head,) * members,
        )
    plans[own] = (((0, rows, rows, False),), [None], (rows,) * members)
    return plans, far, near, own


def sparse_body(members, spectra, top, bottom):
    scans, _, ascans, _ = spectra.shape
    half = members // 2
    tables = tile_tables(TILE)
    plans, far, near, own = exchange_plans(members, scans, ascans)
    stats = jnp.zeros((8, TILE), jnp.float32)
    sent = {}
    peers = far + near + [own]
    for group in tile_groups(far, near, own):
        out = list(send(group, spectra, tables, top, bottom, stats, [plans[p][0] for p in group]))
        for peer in group:
            for level in range(len(plans[peer][0])):
                sent[peer, level] = out.pop(0)
        stats = out.pop(0)
    length = lax.axis_size("scan")
    hops = [("ascan", flipped(members, 1))]
    hops += [("scan", flipped(length, stride)) for stride in strides(length)]
    for axis, pairs in hops:
        stats = stats + lax.ppermute(stats, axis, pairs)
    received, shares = [], [stats]
    for peer in peers:
        for level, pairs in enumerate(plans[peer][1]):
            message = sent[peer, level]
            if pairs is not None:
                message = lax.ppermute(message, "ascan", pairs)
            received.append(message)
    for bits in range(2, members, 2):
        shares.append(lax.ppermute(stats, "ascan", flipped(members, bits)))
    heads = [peers.index(p) for p in far + near]
    starts = np.cumsum([0] + [len(plans[p][0]) for p in peers])
    room = np.zeros((members, TILES, 1), np.float32)
    for peer in peers:
        for source in range(members):
            room[source, int(peer_target(peer, source, half)), 0] = plans[peer][2][source]
    over = judge(
        far + near,
        [plans[p][0][0][2] for p in far + near],
        jnp.asarray(np.broadcast_to(room, (members, TILES, TILE))),
        top,
        bottom,
        [received[starts[i]] for i in heads],
    )

    kernel = functools.partial(receive_kernel, peers, [plans[p][0] for p in peers])
    maps = result_call(kernel, [top, bottom, *received], scans, members * ascans)

    def quick(maps):
        angiogram, mean = finish(maps[0], shares)
        return angiogram, maps[1], maps[2], mean

    def dense(maps):
        out = dense_send(spectra, tables, top, bottom)
        swapped = lax.all_to_all(out, "ascan", 0, 0, tiled=True)
        return result_call(
            dense_receive_kernel,
            [swapped, *shares],
            scans,
            members * ascans,
            [jax.ShapeDtypeStruct((8, TILE), jnp.float32)],
        )

    *outs, mean = lax.cond(over[0, 0] > 0, dense, quick, maps)
    mean_flow = mean[0, 0]
    return (*outs, mean_flow)


def flipped(length, bits):
    return [(s, s ^ bits) for s in range(length)]


def strides(length):
    return [1 << bit for bit in range(length.bit_length() - 1)]


def tile_groups(far, near, own):
    return far[:1], far[1:2], far[2:], near + [own]


def plain_body(spectra, surface_top, surface_bottom):
    scans, repeats, ascans, _ = spectra.shape
    cosine, sine = table_values()
    table = jnp.asarray(np.concatenate([cosine, sine], axis=1).astype(np.float32)).astype(jnp.bfloat16)
    similarity = amplitude_sum = variance = jnp.zeros((scans, ascans, DEPTH), jnp.float32)
    for band in range(BANDS):
        part = spectra[..., band * BAND_BINS : (band + 1) * BAND_BINS]
        profile = jnp.dot(part.reshape(-1, BAND_BINS), table, preferred_element_type=jnp.float32)
        profile = profile.reshape(scans, repeats, ascans, 2 * DEPTH)
        amplitude = jnp.sqrt(profile[..., :DEPTH] ** 2 + profile[..., DEPTH:] ** 2)
        first, second = amplitude[:, :-1], amplitude[:, 1:]
        similarity += jnp.sum(
            2.0 * first * second / jnp.maximum(first**2 + second**2, FLOOR), axis=1
        )
        amplitude_sum += jnp.sum(amplitude, axis=1)
        center = jnp.mean(amplitude, axis=1, keepdims=True)
        variance += jnp.mean((amplitude - center) ** 2, axis=1)
    depth = jnp.arange(DEPTH, dtype=jnp.int32)
    inside = (depth >= surface_top[..., None] * TILE) & (depth < surface_bottom[..., None] * TILE)
    inside = inside.astype(jnp.float32)
    decorrelation = (1.0 - similarity / (BANDS * (REPEATS - 1))) * inside
    structure = amplitude_sum / (BANDS * REPEATS) / math.sqrt(BAND_BINS) * inside
    speckle = variance / BANDS / (VARIANCE_SCALE * BAND_BINS) * inside
    totals = lax.psum((jnp.sum(decorrelation), jnp.sum(inside)), ("scan", "ascan"))
    mean_flow = totals[0] / totals[1]
    decorrelation, structure, speckle = (
        lax.all_to_all(x, "ascan", split_axis=2, concat_axis=1, tiled=True)
        for x in (decorrelation, structure, speckle)
    )
    padded = jnp.pad(decorrelation, ((0, 0), (1, 1), (0, 0)))
    smoothed = (padded[:, :-2] + padded[:, 1:-1] + padded[:, 2:]) / 3.0
    angiogram = jnp.swapaxes(smoothed / mean_flow, 1, 2)
    return (angiogram, jnp.swapaxes(structure, 1, 2), jnp.swapaxes(speckle, 1, 2), mean_flow)


def solution(mesh):
    members = mesh.shape["ascan"]
    scans = mesh.shape["scan"]

    def fits(spectra):
        local_scans, ascans = spectra.shape[0] // scans, spectra.shape[2] // members
        return (
            members == TILES
            and scans & (scans - 1) == 0
            and local_scans % 2 == 0
            and ascans == TILE
            and local_scans * ascans <= MAPS * TILE
        )

    def program(spectra, surface_top, surface_bottom):
        sparse = fits(spectra)
        body = functools.partial(sparse_body, members) if sparse else plain_body
        step = jax.shard_map(
            body,
            mesh=mesh,
            in_specs=(P("scan", None, "ascan", None), P("scan", "ascan"), P("scan", "ascan")),
            out_specs=(
                P("scan", "ascan", None),
                P("scan", "ascan", None),
                P("scan", "ascan", None),
                P(),
            ),
            check_vma=False,
        )
        return step(spectra, surface_top, surface_bottom)

    return program
```
